256 devices in a mesh: tm: 2 (over x_hi), space: 128 (over z, x_lo, y, core).
Axes of the slice: x: 4 (x_hi: 2, x_lo: 2; x = x_hi * 2 + x_lo), y: 4, z: 8, core: 2. Of those that a mesh axis runs over, the one named last changes fastest.
Arguments:
- states: float32 [4, 1024, 64, 128], P('tm', 'space'), may hold values from -1.2 to 1.2
- kappa: float32 [1024, 64, 128], P('space'), may hold values from 0.02 to 0.15
- rate: float32 [1024, 64, 128], P('space'), may hold values from 0.02 to 0.2
Outputs:
- ends: float32 [4, 1024, 64, 128], P('tm', 'space')
The draws below stay inside these ranges and needn't reach their ends.
All inputs are finite; a program needn't handle non-finite values.
Results may differ from the reference program's by a relative error of at most 0.00013.
Values sent between devices are 32-bit elements; how exact they have to be, the bound alone decides.
No kernel may reach another device: no remote copies, remote signals or barrier semaphores. Data moves between devices by JAX's collectives and lax.ppermute only.
A program may use at most 64 MiB of HBM per device.

```python
import math
import jax
import jax.numpy as jnp

NY = 64
NZ = 128
STEPS = 12
COARSE = 3
WINDOWS = 4
NX = 1024


def level_of(key, dims, split, least, largest):
    def one(dim, parts):
        heights = jax.random.uniform(jax.random.fold_in(jax.random.fold_in(key, 6), dim), (parts,), jnp.float32, least / len(split), largest / len(split))
        return jnp.repeat(jnp.exp(heights), dims[dim] // parts).reshape((-1,) + (1,) * (len(dims) - dim - 1))

    gain = one(*split[0])
    for cut in split[1:]:
        gain = gain * one(*cut)
    return gain


def setup_inputs(seed: int = 0) -> dict:
    arg_keys = jax.random.split(jax.random.key(seed), 4)
    return {
        "states": jnp.clip(jax.random.uniform(arg_keys[0], (WINDOWS, NX, NY, NZ), jnp.float32, -1.2, 1.2) * level_of(arg_keys[0], (WINDOWS, NX, NY, NZ), ((0, 2), (1, 128)), -0.4, 0.0), -1.2, 1.2),
        "kappa": jnp.clip(jnp.exp(math.log(0.15) - 2.014903 * jax.random.uniform(arg_keys[1], (NX, NY, NZ), jnp.float32) ** level_of(arg_keys[1], (NX, NY, NZ), ((0, 128),), -0.2, 0.2)), 0.02, 0.15),
        "rate": jnp.clip(jnp.exp(math.log(0.2) - 2.3025851 * jax.random.uniform(arg_keys[2], (NX, NY, NZ), jnp.float32) ** level_of(arg_keys[2], (NX, NY, NZ), ((0, 128),), -0.2, 0.2)), 0.02, 0.2),
    }


def shifted(array, offset):
    lead = array.ndim - 3
    sizes = array.shape[-3:]
    picks = tuple(slice(1 + offset[axis_no], sizes[axis_no] - 1 + offset[axis_no]) for axis_no in range(3))
    return array[(slice(None),) * lead + picks]


def grid_step(field_ext, kappa_ext, rate_mid):
    padded = jnp.pad(field_ext, ((0, 0), (0, 0), (1, 1), (1, 1)))
    kappa_pad = jnp.pad(kappa_ext, ((0, 0), (1, 1), (1, 1)))
    centre = padded[:, 1:-1, 1:-1, 1:-1]
    kappa_mid = kappa_pad[1:-1, 1:-1, 1:-1]
    change = jnp.zeros_like(centre)
    for offset in ((1, 0, 0), (-1, 0, 0), (0, 1, 0), (0, -1, 0), (0, 0, 1), (0, 0, -1)):
        change = change + 0.5 * (kappa_mid + shifted(kappa_pad, offset)) * (shifted(padded, offset) - centre)
    return centre + change + rate_mid * (centre - centre * centre * centre)


def restrict(field_now):
    lead = field_now.shape[:-3]
    sizes = field_now.shape[-3:]
    blocks = field_now.reshape(lead + (sizes[0] // 2, 2, sizes[1] // 2, 2, sizes[2] // 2, 2))
    return jnp.mean(blocks, axis=(-5, -3, -1))


def prolong(coarse_field):
    return jnp.repeat(jnp.repeat(jnp.repeat(coarse_field, 2, axis=-3), 2, axis=-2), 2, axis=-1)


def pad_rows(field_now):
    return jnp.pad(field_now, ((0, 0), (1, 1), (0, 0), (0, 0)))


def reference(states, kappa, rate):
    kappa_ext = jnp.pad(kappa, ((1, 1), (0, 0), (0, 0)))
    fine_end = []
    for window in range(WINDOWS):
        field_now = states[window][None]
        for counter in range(STEPS):
            field_now = grid_step(pad_rows(field_now), kappa_ext, rate)
        fine_end.append(field_now[0])
    coarse_kappa = jnp.pad(restrict(kappa), ((1, 1), (0, 0), (0, 0)))
    coarse_rate = 4.0 * restrict(rate)

    def coarse_prop(coarse_field):
        for sweeps in range(COARSE):
            coarse_field = grid_step(pad_rows(coarse_field), coarse_kappa, coarse_rate)
        return coarse_field

    old_coarse = coarse_prop(restrict(states))
    carried = restrict(states[0:1])
    results = []
    for window in range(WINDOWS):
        moved = coarse_prop(carried)
        results.append(fine_end[window] + prolong(moved[0] - old_coarse[window]))
        carried = (restrict(fine_end[window]) - old_coarse[window])[None] + moved
    return jnp.stack(results)
```

```python
import jax
import jax.numpy as jnp
from jax import lax
from jax.experimental import pallas as pl
from jax.experimental.pallas import tpu as pltpu
from jax.sharding import PartitionSpec as P

F32 = jnp.float32
LANES = 128
PAD = 8
ROWS = 8
BASE = 8
EXT = 24
CROWS = 4
CBASE = 8
CEXT = 20
HALO = 6


def lanes_of(shape):
    return lax.broadcasted_iota(jnp.int32, shape, len(shape) - 1)


def spin(value, shift):
    return pltpu.roll(value, shift % LANES, 1)


def coef_row(i, k_ref, r_ref, coefs, height, zs):
    diag, cx, cy, cz, cw = coefs
    for m in range(height // 8):
        y = PAD + 8 * m
        k = k_ref[i, y : y + 8, :]
        k_next = k_ref[i + 1, y : y + 8, :]
        k_prev = k_ref[i - 1, y : y + 8, :]
        lane = lanes_of(k.shape)
        x_next = 0.5 * (k + k_next)
        x_prev = 0.5 * (k + k_prev)
        y_next = 0.5 * (k + k_ref[i, y + 1 : y + 9, :])
        y_prev = 0.5 * (k + k_ref[i, y - 1 : y + 7, :])
        z_next = jnp.where(lane < LANES - zs, 0.5 * (k + spin(k, -zs)), 0.0)
        z_prev = spin(z_next, zs)
        edge = jnp.where((lane < zs) | (lane >= LANES - zs), 0.5 * k, 0.0)
        total = x_next + x_prev + y_next + y_prev + z_next + z_prev + edge
        diag[i, 8 * m : 8 * m + 8, :] = 1.0 + r_ref[i, y : y + 8, :] - total
        cx[i, 8 * m : 8 * m + 8, :] = jnp.where(jnp.minimum(k, k_next) > 0.0, x_next, 0.0)
        cy[i, y : y + 8, :] = y_next
        cz[i, 8 * m : 8 * m + 8, :] = z_next
        cw[i, 8 * m : 8 * m + 8, :] = z_prev


def build_coefs(k_ref, r_ref, coefs, lo, hi, height, zs):
    diag, cx, cy, cz, cw = coefs
    for m in range(height // 8):
        y = PAD + 8 * m
        k = k_ref[lo - 1, y : y + 8, :]
        k_next = k_ref[lo, y : y + 8, :]
        cx[lo - 1, 8 * m : 8 * m + 8, :] = jnp.where(
            jnp.minimum(k, k_next) > 0.0, 0.5 * (k + k_next), 0.0
        )

    def body(i, carry):
        cy[i, 0:PAD, :] = jnp.zeros((PAD, LANES), F32)
        coef_row(i, k_ref, r_ref, coefs, height, zs)
        return carry

    lax.fori_loop(lo, hi, body, 0)


def advance(src, dst, coefs, r_ref, lo, hi, height, zs, windows, unroll=2):
    diag, cx, cy, cz, cw = coefs

    def body(j, carry):
        for part in range(unroll):
            i = lo + unroll * j + part
            for m in range(height // 8):
                y = PAD + 8 * m
                tile = slice(8 * m, 8 * m + 8)
                a = diag[i, tile, :]
                r = r_ref[i, y : y + 8, :]
                x_next, x_prev = cx[i, tile, :], cx[i - 1, tile, :]
                y_next, y_prev = cy[i, y : y + 8, :], cy[i, y - 1 : y + 7, :]
                z_next, z_prev = cz[i, tile, :], cw[i, tile, :]
                for w in range(windows):
                    u = src[w, i, y : y + 8, :]
                    out = u * (a - r * (u * u))
                    out = out + (x_next * src[w, i + 1, y : y + 8, :] + x_prev * src[w, i - 1, y : y + 8, :])
                    out = out + (y_next * src[w, i, y + 1 : y + 9, :] + y_prev * src[w, i, y - 1 : y + 7, :])
                    out = out + (z_next * spin(u, -zs) + z_prev * spin(u, zs))
                    dst[w, i, y : y + 8, :] = out
        return carry

    lax.fori_loop(0, (hi - lo) // unroll, body, 0)


def clear_pads(ref, lo, hi, height):
    zero = jnp.zeros((PAD, LANES), F32)

    def body(i, carry):
        for lead in range(ref.shape[0]):
            ref[lead, i, 0:PAD, :] = zero
            ref[lead, i, PAD + height : 2 * PAD + height, :] = zero
        return carry

    lax.fori_loop(lo, hi, body, 0)


def clear_pads_flat(ref, lo, hi, height):
    zero = jnp.zeros((PAD, LANES), F32)

    def body(i, carry):
        ref[i, 0:PAD, :] = zero
        ref[i, PAD + height : 2 * PAD + height, :] = zero
        return carry

    lax.fori_loop(lo, hi, body, 0)


def pair_lanes(e):
    even = lanes_of(e.shape) % 2 == 0
    return e + jnp.where(even, spin(e, -1), spin(e, 1))


def coarse_row(load):
    return 0.125 * pair_lanes((load(0, 0) + load(0, 1)) + (load(1, 0) + load(1, 1)))


def pack2(a, b):
    return jnp.where(lanes_of(a.shape) % 2 == 0, a, b)


def unpack_a(v):
    return jnp.where(lanes_of(v.shape) % 2 == 0, v, spin(v, 1))


def unpack_b(v):
    return jnp.where(lanes_of(v.shape) % 2 == 0, spin(v, -1), v)


def odd_here():
    return lax.axis_index("space") % 2


def pack_kernel(states, kappa, rate, send_out, send_in):
    odd = odd_here()
    near_out = 2 * odd
    near_in = 2 - 2 * odd
    for ref, near in ((send_out, near_out), (send_in, near_in)):
        for w in range(2):
            for i in range(HALO):
                ref[HALO * w + i] = states[w, near + i]
        for i in range(ROWS):
            ref[2 * HALO + i] = kappa[i]
            ref[2 * HALO + ROWS + i] = rate[i]


def place_coefs(kappa, rate, got_out, got_in, k_ext, r_ext):
    odd = odd_here()
    at_out = 16 * odd
    at_in = 16 - 16 * odd

    def body(i, carry):
        k_ext[BASE + i, PAD : PAD + 64, :] = kappa[i]
        r_ext[BASE + i, PAD : PAD + 64, :] = rate[i]
        for got, at in ((got_out, at_out), (got_in, at_in)):
            k_ext[at + i, PAD : PAD + 64, :] = got[2 * HALO + i]
            r_ext[at + i, PAD : PAD + 64, :] = got[2 * HALO + ROWS + i]
        return carry

    lax.fori_loop(0, ROWS, body, 0)


def place_states(states, got_out, got_in, field):
    odd = odd_here()
    at_out = 2 + 14 * odd
    at_in = 16 - 14 * odd
    for w in range(2):

        def own(i, carry):
            field[w, BASE + i, PAD : PAD + 64, :] = states[w, i]
            return carry

        def halo(i, carry):
            field[w, at_out + i, PAD : PAD + 64, :] = got_out[HALO * w + i]
            field[w, at_in + i, PAD : PAD + 64, :] = got_in[HALO * w + i]
            return carry

        lax.fori_loop(0, ROWS, own, 0)
        lax.fori_loop(0, HALO, halo, 0)


def lines_of(ref, lead, row):
    return lambda part, first: ref[lead + (row + part, pl.ds(PAD + first, 32, stride=2))]


def first_kernel(states, kappa, rate, got_out, got_in, send, diag, cx, cy, cz, cw, r_ext, k_ext, field, other):
    clear_pads_flat(k_ext, 0, EXT, 64)
    place_coefs(kappa, rate, got_out, got_in, k_ext, r_ext)
    clear_pads(field, 0, EXT, 64)
    clear_pads(other, 0, EXT, 64)
    place_states(states, got_out, got_in, field)
    coefs = (diag, cx, cy, cz, cw)
    build_coefs(k_ext, r_ext, coefs, 1, EXT - 1, 64, 1)
    src, dst = field, other
    for n in range(6):
        reach = 5 - n
        advance(src, dst, coefs, r_ext, BASE - reach, BASE + ROWS + reach, 64, 1, 2)
        src, dst = dst, src
    for w in range(2):
        for i in range(ROWS):
            send[ROWS * w + i] = src[w, BASE + i, PAD : PAD + 64, :]
    for slot, row in enumerate((-2, -1, 4, 5)):
        fine = BASE + 2 * row
        packed = pack2(
            coarse_row(lines_of(k_ext, (), fine)), 4.0 * coarse_row(lines_of(r_ext, (), fine))
        )
        send[16 + slot // 2, 32 * (slot % 2) : 32 * (slot % 2) + 32, :] = packed


def old_kernel(states, got_out, got_in, k_ext, r_ext, old, kc, rc, field, diag, cx, cy, cz, cw, here, there):
    place_states(states, got_out, got_in, field)
    clear_pads_flat(kc, 0, CEXT, 32)
    clear_pads(here, 0, CEXT, 32)
    clear_pads(there, 0, CEXT, 32)

    def row_coefs(i, carry):
        kc[CBASE - 4 + i, PAD : PAD + 32, :] = coarse_row(lines_of(k_ext, (), 2 * i))
        rc[CBASE - 4 + i, PAD : PAD + 32, :] = 4.0 * coarse_row(lines_of(r_ext, (), 2 * i))
        return carry

    lax.fori_loop(0, 12, row_coefs, 0)

    def row_states(i, carry):
        for w in range(2):
            here[w, CBASE - 3 + i, PAD : PAD + 32, :] = coarse_row(lines_of(field, (w,), 2 + 2 * i))
        return carry

    lax.fori_loop(0, 10, row_states, 0)
    coefs = (diag, cx, cy, cz, cw)
    build_coefs(kc, rc, coefs, CBASE - 2, CBASE + CROWS + 2, 32, 2)
    src, dst = here, there
    for n in range(3):
        reach = 2 - n
        advance(src, dst, coefs, rc, CBASE - reach, CBASE + CROWS + reach, 32, 2, 2)
        src, dst = dst, src
    for w in range(2):
        for i in range(CROWS):
            old[w, i] = src[w, CBASE + i, PAD : PAD + 32, :]


def second_kernel(
    sent, got_out, got_in, diag, cx, cy, cz, cw, r_ext, old, fine_end, send, field, other
):
    odd = odd_here()
    clear_pads(field, 0, EXT, 64)
    clear_pads(other, 0, EXT, 64)
    for w in range(2):

        def own(i, carry):
            field[w, BASE + i, PAD : PAD + 64, :] = sent[ROWS * w + i]
            field[w, 16 * odd + i, PAD : PAD + 64, :] = got_out[ROWS * w + i]
            field[w, 16 - 16 * odd + i, PAD : PAD + 64, :] = got_in[ROWS * w + i]
            return carry

        lax.fori_loop(0, ROWS, own, 0)
    coefs = (diag, cx, cy, cz, cw)
    src, dst = field, other
    for n in range(6):
        reach = 7 - n
        advance(src, dst, coefs, r_ext, BASE - reach, BASE + ROWS + reach, 64, 1, 2)
        src, dst = dst, src
    later = (lax.axis_index("tm") > 0).astype(F32)
    for i in range(-1, 5):
        rows = []
        for w in range(2):
            value = coarse_row(lines_of(src, (w,), BASE + 2 * i))
            if 0 <= i < CROWS:
                value = value - (old[w, i] if w else later * old[w, i])
            rows.append(value)
        send[1 + i] = pack2(*rows)
    for w in range(2):
        for i in range(ROWS):
            fine_end[w, i] = src[w, BASE + i, PAD : PAD + 64, :]


def third_kernel(
    sent, got_out, got_in, kc_near, rc_near, sent2, got_out2, got_in2,
    tm_mid, tm_up, tm_down, first, newer, rc, diag, cx, cy, cz, cw, kc, here, there,
):
    odd = odd_here()
    clear_pads_flat(kc, 0, CEXT, 32)
    clear_pads(here, 0, CEXT, 32)
    clear_pads(there, 0, CEXT, 32)

    def near(i, carry):
        kc[i, PAD : PAD + 32, :] = kc_near[i, PAD : PAD + 32, :]
        rc[i, PAD : PAD + 32, :] = rc_near[i, PAD : PAD + 32, :]
        return carry

    lax.fori_loop(CBASE - 4, CBASE + 8, near, 0)
    for got, above in ((got_out2, odd), (got_in2, 1 - odd)):
        for j in range(2):
            packed = got[16 + above, 32 * j : 32 * j + 32, :]
            row = CBASE - 6 + 14 * above + j
            kc[row, PAD : PAD + 32, :] = unpack_a(packed)
            rc[row, PAD : PAD + 32, :] = unpack_b(packed)
    coefs = (diag, cx, cy, cz, cw)
    build_coefs(kc, rc, coefs, CBASE - 5, CBASE + CROWS + 5, 32, 2)

    for i in range(CROWS):
        here[0, CBASE + i, PAD : PAD + 32, :] = unpack_a(sent[1 + i])
        there[1, CBASE + i, PAD : PAD + 32, :] = unpack_b(sent[1 + i])
    for got, above in ((got_out, odd), (got_in, 1 - odd)):
        for j in range(5):
            packed = got[above + j]
            row = CBASE - 5 + 9 * above + j
            here[0, row, PAD : PAD + 32, :] = unpack_a(packed)
            there[1, row, PAD : PAD + 32, :] = unpack_b(packed)
    for i in range(-3, 7):
        first[3 + i] = here[0, CBASE + i, PAD : PAD + 32, :]
    advance(here, there, coefs, rc, CBASE - 4, CBASE + CROWS + 4, 32, 2, 1)
    advance(there, here, coefs, rc, CBASE - 3, CBASE + CROWS + 3, 32, 2, 1)
    advance(here, there, coefs, rc, CBASE - 2, CBASE + CROWS + 2, 32, 2, 1)
    carried = []
    for i in range(-2, 6):
        moved = there[0, CBASE + i, PAD : PAD + 32, :]
        if 0 <= i < CROWS:
            newer[i] = moved
        carried.append(moved + there[1, CBASE + i, PAD : PAD + 32, :])
    for j in range(4):
        tm_mid[j] = pack2(carried[2 * j], carried[2 * j + 1])
    for j in range(2):
        tm_up[j] = pack2(carried[2 * j], carried[2 * j + 1])
        tm_down[j] = pack2(carried[4 + 2 * j], carried[5 + 2 * j])


def last_kernel(
    fine_end, old, first, newer, tm_mid, from_below, from_above, rc, diag, cx, cy, cz, cw, ends, here, there
):
    clear_pads(here, 0, CEXT, 32)
    clear_pads(there, 0, CEXT, 32)
    for ref, start, count in ((from_below, -6, 2), (tm_mid, -2, 4), (from_above, 6, 2)):
        for j in range(count):
            row = CBASE + start + 2 * j
            here[0, row, PAD : PAD + 32, :] = unpack_a(ref[j])
            here[0, row + 1, PAD : PAD + 32, :] = unpack_b(ref[j])
    coefs = (diag, cx, cy, cz, cw)
    advance(here, there, coefs, rc, CBASE - 5, CBASE + CROWS + 5, 32, 2, 1)
    advance(there, here, coefs, rc, CBASE - 4, CBASE + CROWS + 4, 32, 2, 1)
    advance(here, there, coefs, rc, CBASE - 3, CBASE + CROWS + 3, 32, 2, 1)
    second = []
    for i in range(-3, 7):
        moved = there[0, CBASE + i, PAD : PAD + 32, :]
        if 0 <= i < CROWS:
            second.append(moved)
        here[0, CBASE + i, PAD : PAD + 32, :] = first[3 + i] + moved
    advance(here, there, coefs, rc, CBASE - 2, CBASE + CROWS + 2, 32, 2, 1)
    advance(there, here, coefs, rc, CBASE - 1, CBASE + CROWS + 1, 32, 2, 1)
    advance(here, there, coefs, rc, CBASE, CBASE + CROWS, 32, 2, 1)
    later = lax.axis_index("tm") > 0
    for i in range(CROWS):
        third = there[0, CBASE + i, PAD : PAD + 32, :]
        shifts = (
            jnp.where(later, second[i] - old[0, i], 0.0),
            jnp.where(later, third, newer[i]) - old[1, i],
        )
        for w in range(2):
            for part in range(2):
                for line in range(2):
                    lines = pl.ds(line, 32, stride=2)
                    ends[w, 2 * i + part, lines, :] = fine_end[w, 2 * i + part, lines, :] + shifts[w]


def shape(*sizes):
    return jax.ShapeDtypeStruct(sizes, F32)


def call(kernel, outs, scratch, flops, *args):
    return pl.pallas_call(
        kernel,
        out_shape=outs,
        in_specs=[pl.BlockSpec(memory_space=pltpu.VMEM)] * len(args),
        out_specs=[pl.BlockSpec(memory_space=pltpu.VMEM)] * len(outs),
        scratch_shapes=[pltpu.VMEM(sizes, F32) for sizes in scratch],
        compiler_params=pltpu.CompilerParams(vmem_limit_bytes=24 * 1024 * 1024),
        cost_estimate=pl.CostEstimate(flops=flops, bytes_accessed=1 << 20, transcendentals=0),
    )(*args)


def swap(value, odd_pairs):
    count, groups = lax.axis_size("space"), lax.axis_size("tm")
    pairs = []
    for group in range(groups):
        for low in range(1 if odd_pairs else 0, count - 1, 2):
            a, b = group * count + low, group * count + low + 1
            pairs += [(a, b), (b, a)]
    return lax.ppermute(value, ("tm", "space"), pairs)


def over_tm(value, offset):
    count = lax.axis_size("space")
    pairs = [(s, count + s + offset) for s in range(count) if 0 <= s + offset < count]
    return lax.ppermute(value, ("tm", "space"), pairs)


FINE_COEFS = [(EXT, 64, LANES), (EXT, 64, LANES), (EXT, 64 + 2 * PAD, LANES), (EXT, 64, LANES), (EXT, 64, LANES)]
COARSE_COEFS = [(CEXT, 32, LANES), (CEXT, 32, LANES), (CEXT, 32 + 2 * PAD, LANES), (CEXT, 32, LANES), (CEXT, 32, LANES)]
FINE_FIELD = (2, EXT, 64 + 2 * PAD, LANES)
FINE_FLAT = (EXT, 64 + 2 * PAD, LANES)
COARSE_FIELD = (2, CEXT, 32 + 2 * PAD, LANES)
COARSE_FLAT = (CEXT, 32 + 2 * PAD, LANES)


def shards(states, kappa, rate):
    units = 2 * HALO + 2 * ROWS
    send_out, send_in = call(
        pack_kernel, [shape(units, 64, LANES)] * 2, [], 1000, states, kappa, rate
    )
    got_out, got_in = swap(send_out, True), swap(send_in, False)
    send, diag, cx, cy, cz, cw, r_ext, k_ext = call(
        first_kernel,
        [shape(18, 64, LANES)] + [shape(*s) for s in FINE_COEFS] + [shape(*FINE_FLAT)] * 2,
        [FINE_FIELD] * 2,
        10_000_000,
        states, kappa, rate, got_out, got_in,
    )
    got_out2, got_in2 = swap(send, True), swap(send, False)
    old, kc, rc = call(
        old_kernel,
        [shape(2, CROWS, 32, LANES), shape(*COARSE_FLAT), shape(*COARSE_FLAT)],
        [FINE_FIELD] + COARSE_COEFS + [COARSE_FIELD] * 2,
        10_000_000,
        states, got_out, got_in, k_ext, r_ext,
    )
    fine_end, send3 = call(
        second_kernel,
        [shape(2, ROWS, 64, LANES), shape(6, 32, LANES)],
        [FINE_FIELD] * 2,
        10_000_000,
        send, got_out2, got_in2, diag, cx, cy, cz, cw, r_ext, old,
    )
    got_out3, got_in3 = swap(send3, True), swap(send3, False)
    tm_mid, tm_up, tm_down, first, newer, rc2, *coarse = call(
        third_kernel,
        [shape(4, 32, LANES), shape(2, 32, LANES), shape(2, 32, LANES), shape(10, 32, LANES), shape(CROWS, 32, LANES)]
        + [shape(*COARSE_FLAT)] + [shape(*s) for s in COARSE_COEFS],
        [COARSE_FLAT] + [COARSE_FIELD] * 2,
        10_000_000,
        send3, got_out3, got_in3, kc, rc, send, got_out2, got_in2,
    )
    mid, from_below, from_above = over_tm(tm_mid, 0), over_tm(tm_up, 1), over_tm(tm_down, -1)
    (ends,) = call(
        last_kernel,
        [shape(2, ROWS, 64, LANES)],
        [COARSE_FIELD] * 2,
        10_000_000,
        fine_end, old, first, newer, mid, from_below, from_above, rc2, *coarse,
    )
    return ends


def solution(mesh):
    in_specs = (P("tm", "space", None, None), P("space", None, None), P("space", None, None))
    out_specs = P("tm", "space", None, None)
    return jax.shard_map(shards, mesh=mesh, in_specs=in_specs, out_specs=out_specs, check_vma=False)
```

```python
import jax
import jax.numpy as jnp
from jax import lax
from jax.experimental import pallas as pl
from jax.experimental.pallas import tpu as pltpu
from jax.sharding import PartitionSpec as P

F32 = jnp.float32
LANES = 128
PAD = 8
ROWS = 8
BASE = 8
EXT = 24
CROWS = 4
CBASE = 8
CEXT = 20
HALO = 6


def lanes_of(shape):
    return lax.broadcasted_iota(jnp.int32, shape, len(shape) - 1)


def spin(value, shift):
    return pltpu.roll(value, shift % LANES, 1)


def coef_tile(i, m, k_ref, r_ref, coefs, zs):
    diag, cx, cy, cz, cw = coefs
    y = PAD + 8 * m
    k = k_ref[i, y : y + 8, :]
    k_next = k_ref[i + 1, y : y + 8, :]
    k_prev = k_ref[i - 1, y : y + 8, :]
    lane = lanes_of(k.shape)
    x_next = 0.5 * (k + k_next)
    x_prev = 0.5 * (k + k_prev)
    y_next = 0.5 * (k + k_ref[i, y + 1 : y + 9, :])
    y_prev = 0.5 * (k + k_ref[i, y - 1 : y + 7, :])
    z_next = jnp.where(lane < LANES - zs, 0.5 * (k + spin(k, -zs)), 0.0)
    z_prev = jnp.where(lane >= zs, 0.5 * (k + spin(k, zs)), 0.0)
    edge = jnp.where((lane < zs) | (lane >= LANES - zs), 0.5 * k, 0.0)
    total = x_next + x_prev + y_next + y_prev + z_next + z_prev + edge
    diag[i, 8 * m : 8 * m + 8, :] = 1.0 + r_ref[i, y : y + 8, :] - total
    cx[i, 8 * m : 8 * m + 8, :] = jnp.where(jnp.minimum(k, k_next) > 0.0, x_next, 0.0)
    cy[i, y : y + 8, :] = y_next
    cz[i, 8 * m : 8 * m + 8, :] = z_next
    cw[i, 8 * m : 8 * m + 8, :] = z_prev


def blocks(count, unroll, block):
    if count <= unroll:
        block(0, count)
        return
    trips = -(-count // unroll)
    rows = -(-count // trips)
    whole = count // rows

    def body(j, carry):
        block(j * rows, rows)
        return carry

    lax.fori_loop(0, whole, body, 0)
    if count - whole * rows:
        block(whole * rows, count - whole * rows)


def build_coefs(k_ref, r_ref, coefs, lo, count, height, zs):
    _, cx, cy, _, _ = coefs
    for m in range(height // 8):
        y = PAD + 8 * m
        k = k_ref[lo - 1, y : y + 8, :]
        k_next = k_ref[lo, y : y + 8, :]
        cx[lo - 1, 8 * m : 8 * m + 8, :] = jnp.where(
            jnp.minimum(k, k_next) > 0.0, 0.5 * (k + k_next), 0.0
        )

    def block(first, rows):
        for i in range(rows):
            cy[lo + first + i, 0:PAD, :] = jnp.zeros((PAD, LANES), F32)
            for m in range(height // 8):
                coef_tile(lo + first + i, m, k_ref, r_ref, coefs, zs)

    blocks(count, 8 if height == 64 else 14, block)


def advance(src, dst, coefs, r_ref, lo, count, height, zs, windows, unroll=8):
    diag, cx, cy, cz, cw = coefs

    def block(first, rows):
        base = lo + first
        for m in range(height // 8):
            y = PAD + 8 * m
            here = slice(y, y + 8)
            tile = slice(8 * m, 8 * m + 8)
            line = [[src[w, base + i, here, :] for i in range(-1, rows + 1)] for w in range(windows)]
            across = [cx[base + i, tile, :] for i in range(-1, rows)]
            for i in range(rows):
                row = base + i
                a = diag[row, tile, :]
                r = r_ref[row, here, :]
                y_next, y_prev = cy[row, here, :], cy[row, y - 1 : y + 7, :]
                z_next, z_prev = cz[row, tile, :], cw[row, tile, :]
                for w in range(windows):
                    u = line[w][i + 1]
                    out = u * (a - r * (u * u))
                    out = out + (across[i + 1] * line[w][i + 2] + across[i] * line[w][i])
                    out = out + (y_next * src[w, row, y + 1 : y + 9, :] + y_prev * src[w, row, y - 1 : y + 7, :])
                    out = out + (z_next * spin(u, -zs) + z_prev * spin(u, zs))
                    dst[w, row, here, :] = out

    blocks(count, unroll, block)


def clear_pads(ref, lo, hi, height):
    zero = jnp.zeros((PAD, LANES), F32)

    def body(i, carry):
        for lead in range(ref.shape[0]):
            ref[lead, i, 0:PAD, :] = zero
            ref[lead, i, PAD + height : 2 * PAD + height, :] = zero
        return carry

    lax.fori_loop(lo, hi, body, 0)


def clear_pads_flat(ref, lo, hi, height):
    zero = jnp.zeros((PAD, LANES), F32)

    def body(i, carry):
        ref[i, 0:PAD, :] = zero
        ref[i, PAD + height : 2 * PAD + height, :] = zero
        return carry

    lax.fori_loop(lo, hi, body, 0)


def pair_lanes(e):
    even = lanes_of(e.shape) % 2 == 0
    return e + jnp.where(even, spin(e, -1), spin(e, 1))


def coarse_row(load):
    return 0.125 * pair_lanes((load(0, 0) + load(0, 1)) + (load(1, 0) + load(1, 1)))


def pack2(a, b):
    return jnp.where(lanes_of(a.shape) % 2 == 0, a, b)


def unpack_a(v):
    return jnp.where(lanes_of(v.shape) % 2 == 0, v, spin(v, 1))


def unpack_b(v):
    return jnp.where(lanes_of(v.shape) % 2 == 0, spin(v, -1), v)


def odd_here():
    return lax.axis_index("space") % 2


def pack_kernel(states, kappa, rate, send_out, send_in):
    odd = odd_here()
    for ref, near in ((send_out, 2 * odd), (send_in, 2 - 2 * odd)):
        for w in range(2):
            for i in range(HALO):
                ref[HALO * w + i] = states[w, near + i]
        for i in range(ROWS):
            ref[2 * HALO + i] = kappa[i]
            ref[2 * HALO + ROWS + i] = rate[i]


def place_halo(got, field, k_ext, r_ext, above):
    for w in range(2):

        def halo(i, carry):
            field[w, 2 + 14 * above + i, PAD : PAD + 64, :] = got[HALO * w + i]
            return carry

        lax.fori_loop(0, HALO, halo, 0)

    def coef(i, carry):
        k_ext[16 * above + i, PAD : PAD + 64, :] = got[2 * HALO + i]
        r_ext[16 * above + i, PAD : PAD + 64, :] = got[2 * HALO + ROWS + i]
        return carry

    lax.fori_loop(0, ROWS, coef, 0)


def place_own(states, field):
    def own(i, carry):
        for w in range(2):
            field[w, BASE + i, PAD : PAD + 64, :] = states[w, i]
        return carry

    lax.fori_loop(0, ROWS, own, 0)


def lines_of(ref, lead, row):
    return lambda part, first: ref[lead + (row + part, pl.ds(PAD + first, 32, stride=2))]


def inner_first_kernel(states, kappa, rate, got_in, field, other, diag, cx, cy, cz, cw, r_ext, k_ext):
    odd = odd_here()
    clear_pads_flat(k_ext, 0, EXT, 64)
    clear_pads(field, 0, EXT, 64)
    clear_pads(other, 0, EXT, 64)
    place_own(states, field)

    def own(i, carry):
        k_ext[BASE + i, PAD : PAD + 64, :] = kappa[i]
        r_ext[BASE + i, PAD : PAD + 64, :] = rate[i]
        return carry

    lax.fori_loop(0, ROWS, own, 0)
    place_halo(got_in, field, k_ext, r_ext, 1 - odd)
    coefs = (diag, cx, cy, cz, cw)
    build_coefs(k_ext, r_ext, coefs, 9 - 8 * odd, 14, 64, 1)
    src, dst = field, other
    for n in range(1, 7):
        advance(src, dst, coefs, r_ext, BASE + n - 6 * odd, 14 - 2 * n, 64, 1, 2)
        src, dst = dst, src


def outer_first_kernel(got_out, *refs):
    refs = refs[9:]
    send, field, other, diag, cx, cy, cz, cw, r_ext, k_ext = refs
    odd = odd_here()
    place_halo(got_out, field, k_ext, r_ext, odd)
    coefs = (diag, cx, cy, cz, cw)
    build_coefs(k_ext, r_ext, coefs, 1 + 14 * odd, 8, 64, 1)
    src, dst = field, other
    for n in range(1, 7):
        advance(src, dst, coefs, r_ext, 2 + n + (14 - 2 * n) * odd, 6, 64, 1, 2)
        src, dst = dst, src

    def own(i, carry):
        for w in range(2):
            send[ROWS * w + i] = src[w, BASE + i, PAD : PAD + 64, :]
        return carry

    lax.fori_loop(0, ROWS, own, 0)
    for slot, row in enumerate((-2, -1, 4, 5)):
        fine = BASE + 2 * row
        packed = pack2(
            coarse_row(lines_of(k_ext, (), fine)), 4.0 * coarse_row(lines_of(r_ext, (), fine))
        )
        send[16 + slot // 2, 32 * (slot % 2) : 32 * (slot % 2) + 32, :] = packed


def inner_second_kernel(got_in, *refs):
    _, _, diag, cx, cy, cz, cw, r_ext, field, other = refs
    odd = odd_here()

    def halo(i, carry):
        for w in range(2):
            field[w, 16 - 16 * odd + i, PAD : PAD + 64, :] = got_in[ROWS * w + i]
        return carry

    lax.fori_loop(0, ROWS, halo, 0)
    coefs = (diag, cx, cy, cz, cw)
    src, dst = field, other
    for n in range(1, 7):
        advance(src, dst, coefs, r_ext, BASE + n - 8 * odd, 16 - 2 * n, 64, 1, 2)
        src, dst = dst, src


def outer_second_kernel(got_out, *refs):
    _, _, diag, cx, cy, cz, cw, r_ext, old, field, other, send = refs
    odd = odd_here()

    def halo(i, carry):
        for w in range(2):
            field[w, 16 * odd + i, PAD : PAD + 64, :] = got_out[ROWS * w + i]
        return carry

    lax.fori_loop(0, ROWS, halo, 0)
    coefs = (diag, cx, cy, cz, cw)
    src, dst = field, other
    for n in range(1, 7):
        advance(src, dst, coefs, r_ext, n + (16 - 2 * n) * odd, 8, 64, 1, 2)
        src, dst = dst, src
    later = (lax.axis_index("tm") > 0).astype(F32)
    for i in range(-1, 5):
        rows = []
        for w in range(2):
            value = coarse_row(lines_of(src, (w,), BASE + 2 * i))
            if 0 <= i < CROWS:
                value = value - (old[w, i] if w else later * old[w, i])
            rows.append(value)
        send[1 + i] = pack2(*rows)


def old_kernel(states, got_out, got_in, k_ext, r_ext, old, kc, rc, field, diag, cx, cy, cz, cw, here, there):
    odd = odd_here()
    place_own(states, field)
    for got, above in ((got_out, odd), (got_in, 1 - odd)):
        for w in range(2):

            def halo(i, carry):
                field[w, 2 + 14 * above + i, PAD : PAD + 64, :] = got[HALO * w + i]
                return carry

            lax.fori_loop(0, HALO, halo, 0)
    clear_pads_flat(kc, 0, CEXT, 32)
    clear_pads(here, 0, CEXT, 32)
    clear_pads(there, 0, CEXT, 32)

    def row_coefs(first, rows):
        for i in range(rows):
            at = first + i
            kc[CBASE - 4 + at, PAD : PAD + 32, :] = coarse_row(lines_of(k_ext, (), 2 * at))
            rc[CBASE - 4 + at, PAD : PAD + 32, :] = 4.0 * coarse_row(lines_of(r_ext, (), 2 * at))

    blocks(12, 6, row_coefs)

    def row_states(first, rows):
        for i in range(rows):
            for w in range(2):
                value = coarse_row(lines_of(field, (w,), 2 + 2 * (first + i)))
                here[w, CBASE - 3 + first + i, PAD : PAD + 32, :] = value

    blocks(10, 5, row_states)
    coefs = (diag, cx, cy, cz, cw)
    build_coefs(kc, rc, coefs, CBASE - 2, CROWS + 4, 32, 2)
    src, dst = here, there
    for n in range(3):
        reach = 2 - n
        advance(src, dst, coefs, rc, CBASE - reach, CROWS + 2 * reach, 32, 2, 2)
        src, dst = dst, src
    for w in range(2):
        for i in range(CROWS):
            old[w, i] = src[w, CBASE + i, PAD : PAD + 32, :]


def chain_coefs_kernel(kc_near, rc_near, sent2, got_out2, got_in2, rc, diag, cx, cy, cz, cw, kc):
    odd = odd_here()
    clear_pads_flat(kc, 0, CEXT, 32)

    def near(i, carry):
        kc[i, PAD : PAD + 32, :] = kc_near[i, PAD : PAD + 32, :]
        rc[i, PAD : PAD + 32, :] = rc_near[i, PAD : PAD + 32, :]
        return carry

    lax.fori_loop(CBASE - 4, CBASE + 8, near, 0)
    for got, above in ((got_out2, odd), (got_in2, 1 - odd)):
        for j in range(2):
            packed = got[16 + above, 32 * j : 32 * j + 32, :]
            row = CBASE - 6 + 14 * above + j
            kc[row, PAD : PAD + 32, :] = unpack_a(packed)
            rc[row, PAD : PAD + 32, :] = unpack_b(packed)
    build_coefs(kc, rc, (diag, cx, cy, cz, cw), CBASE - 5, CROWS + 10, 32, 2)


def third_kernel(
    sent, got_out, got_in, rc, diag, cx, cy, cz, cw,
    tm_mid, tm_up, tm_down, first, newer, here, there,
):
    odd = odd_here()
    clear_pads(here, 0, CEXT, 32)
    clear_pads(there, 0, CEXT, 32)
    coefs = (diag, cx, cy, cz, cw)
    for i in range(CROWS):
        here[0, CBASE + i, PAD : PAD + 32, :] = unpack_a(sent[1 + i])
        there[1, CBASE + i, PAD : PAD + 32, :] = unpack_b(sent[1 + i])
    for got, above in ((got_out, odd), (got_in, 1 - odd)):
        for j in range(5):
            packed = got[above + j]
            row = CBASE - 5 + 9 * above + j
            here[0, row, PAD : PAD + 32, :] = unpack_a(packed)
            there[1, row, PAD : PAD + 32, :] = unpack_b(packed)
    for i in range(-3, 7):
        first[3 + i] = here[0, CBASE + i, PAD : PAD + 32, :]
    advance(here, there, coefs, rc, CBASE - 4, CROWS + 8, 32, 2, 1, 14)
    advance(there, here, coefs, rc, CBASE - 3, CROWS + 6, 32, 2, 1, 14)
    advance(here, there, coefs, rc, CBASE - 2, CROWS + 4, 32, 2, 1, 14)
    carried = []
    for i in range(-2, 6):
        moved = there[0, CBASE + i, PAD : PAD + 32, :]
        if 0 <= i < CROWS:
            newer[i] = moved
        carried.append(moved + there[1, CBASE + i, PAD : PAD + 32, :])
    for j in range(4):
        tm_mid[j] = pack2(carried[2 * j], carried[2 * j + 1])
    for j in range(2):
        tm_up[j] = pack2(carried[2 * j], carried[2 * j + 1])
        tm_down[j] = pack2(carried[4 + 2 * j], carried[5 + 2 * j])


def last_kernel(
    fine, old, first, newer, tm_mid, from_below, from_above, rc, diag, cx, cy, cz, cw, ends, here, there
):
    clear_pads(here, 0, CEXT, 32)
    clear_pads(there, 0, CEXT, 32)
    for ref, start, count in ((from_below, -6, 2), (tm_mid, -2, 4), (from_above, 6, 2)):
        for j in range(count):
            row = CBASE + start + 2 * j
            here[0, row, PAD : PAD + 32, :] = unpack_a(ref[j])
            here[0, row + 1, PAD : PAD + 32, :] = unpack_b(ref[j])
    coefs = (diag, cx, cy, cz, cw)
    advance(here, there, coefs, rc, CBASE - 5, CROWS + 10, 32, 2, 1, 14)
    advance(there, here, coefs, rc, CBASE - 4, CROWS + 8, 32, 2, 1, 14)
    advance(here, there, coefs, rc, CBASE - 3, CROWS + 6, 32, 2, 1, 14)
    second = []
    for i in range(-3, 7):
        moved = there[0, CBASE + i, PAD : PAD + 32, :]
        if 0 <= i < CROWS:
            second.append(moved)
        here[0, CBASE + i, PAD : PAD + 32, :] = first[3 + i] + moved
    advance(here, there, coefs, rc, CBASE - 2, CROWS + 4, 32, 2, 1, 14)
    advance(there, here, coefs, rc, CBASE - 1, CROWS + 2, 32, 2, 1, 14)
    advance(here, there, coefs, rc, CBASE, CROWS, 32, 2, 1, 14)
    later = lax.axis_index("tm") > 0
    for i in range(CROWS):
        third = there[0, CBASE + i, PAD : PAD + 32, :]
        shifts = (
            jnp.where(later, second[i] - old[0, i], 0.0),
            jnp.where(later, third, newer[i]) - old[1, i],
        )
        for w in range(2):
            for part in range(2):
                for line in range(2):
                    value = fine[w, BASE + 2 * i + part, pl.ds(PAD + line, 32, stride=2), :]
                    ends[w, 2 * i + part, pl.ds(line, 32, stride=2), :] = value + shifts[w]


def shape(*sizes):
    return jax.ShapeDtypeStruct(sizes, F32)


def call(kernel, outs, scratch, cost, *args, aliases=None):
    return pl.pallas_call(
        kernel,
        out_shape=outs,
        in_specs=[pl.BlockSpec(memory_space=pltpu.VMEM)] * len(args),
        out_specs=[pl.BlockSpec(memory_space=pltpu.VMEM)] * len(outs),
        scratch_shapes=[pltpu.VMEM(sizes, F32) for sizes in scratch],
        input_output_aliases=aliases or {},
        compiler_params=pltpu.CompilerParams(vmem_limit_bytes=24 * 1024 * 1024),
        cost_estimate=pl.CostEstimate(flops=cost, bytes_accessed=1 << 20, transcendentals=0),
    )(*args)


def swap(value, odd_pairs):
    count, groups = lax.axis_size("space"), lax.axis_size("tm")
    pairs = []
    for group in range(groups):
        for low in range(1 if odd_pairs else 0, count - 1, 2):
            a, b = group * count + low, group * count + low + 1
            pairs += [(a, b), (b, a)]
    return lax.ppermute(value, ("tm", "space"), pairs)


def over_tm(value, offset):
    count = lax.axis_size("space")
    pairs = [(s, count + s + offset) for s in range(count) if 0 <= s + offset < count]
    return lax.ppermute(value, ("tm", "space"), pairs)


FINE_COEFS = [(EXT, 64, LANES), (EXT, 64, LANES), (EXT, 64 + 2 * PAD, LANES), (EXT, 64, LANES), (EXT, 64, LANES)]
COARSE_COEFS = [(CEXT, 32, LANES), (CEXT, 32, LANES), (CEXT, 32 + 2 * PAD, LANES), (CEXT, 32, LANES), (CEXT, 32, LANES)]
FINE_FIELD = (2, EXT, 64 + 2 * PAD, LANES)
FINE_FLAT = (EXT, 64 + 2 * PAD, LANES)
COARSE_FIELD = (2, CEXT, 32 + 2 * PAD, LANES)
COARSE_FLAT = (CEXT, 32 + 2 * PAD, LANES)


def swaps(value_out, value_in):
    got_out = swap(value_out, True)
    got_in = swap(value_in, False)
    return got_out, got_in


COST = 10_000_000


def shards(states, kappa, rate):
    units = 2 * HALO + 2 * ROWS
    fields = [shape(*FINE_FIELD)] * 2
    fine_coefs = [shape(*sizes) for sizes in FINE_COEFS]
    coarse_coefs = [shape(*sizes) for sizes in COARSE_COEFS]
    send_out, send_in = call(
        pack_kernel, [shape(units, 64, LANES)] * 2, [], 1000, states, kappa, rate
    )
    got_out, got_in = swaps(send_out, send_in)
    work = call(
        inner_first_kernel,
        fields + fine_coefs + [shape(*FINE_FLAT)] * 2,
        [], COST, states, kappa, rate, got_in,
    )
    send, *work = call(
        outer_first_kernel,
        [shape(18, 64, LANES)] + fields + fine_coefs + [shape(*FINE_FLAT)] * 2,
        [], COST, got_out, *work, aliases={1 + n: 1 + n for n in range(9)},
    )
    field, other, *coefs, r_ext, k_ext = work
    got_out2, got_in2 = swaps(send, send)
    old, kc, rc = call(
        old_kernel,
        [shape(2, CROWS, 32, LANES), shape(*COARSE_FLAT), shape(*COARSE_FLAT)],
        [FINE_FIELD] + COARSE_COEFS + [COARSE_FIELD] * 2,
        COST, states, got_out, got_in, k_ext, r_ext,
    )
    field, other = call(
        inner_second_kernel, fields, [], COST, got_in2, field, other, *coefs, r_ext,
        aliases={1: 0, 2: 1},
    )
    field, other, send3 = call(
        outer_second_kernel,
        fields + [shape(6, 32, LANES)],
        [], COST, got_out2, field, other, *coefs, r_ext, old, aliases={1: 0, 2: 1},
    )
    got_out3, got_in3 = swaps(send3, send3)
    rc2, *coarse = call(
        chain_coefs_kernel, [shape(*COARSE_FLAT)] + coarse_coefs, [COARSE_FLAT],
        COST, kc, rc, send, got_out2, got_in2,
    )
    tm_mid, tm_up, tm_down, first, newer = call(
        third_kernel,
        [shape(4, 32, LANES), shape(2, 32, LANES), shape(2, 32, LANES), shape(10, 32, LANES), shape(CROWS, 32, LANES)],
        [COARSE_FIELD] * 2,
        COST, send3, got_out3, got_in3, rc2, *coarse,
    )
    mid, from_below, from_above = over_tm(tm_mid, 0), over_tm(tm_up, 1), over_tm(tm_down, -1)
    (ends,) = call(
        last_kernel,
        [shape(2, ROWS, 64, LANES)],
        [COARSE_FIELD] * 2,
        COST, field, old, first, newer, mid, from_below, from_above, rc2, *coarse,
    )
    return ends


def solution(mesh):
    in_specs = (P("tm", "space", None, None), P("space", None, None), P("space", None, None))
    out_specs = P("tm", "space", None, None)
    return jax.shard_map(shards, mesh=mesh, in_specs=in_specs, out_specs=out_specs, check_vma=False)
```

```python
import jax
import jax.numpy as jnp
from jax import lax
from jax.experimental import pallas as pl
from jax.experimental.pallas import tpu as pltpu
from jax.sharding import PartitionSpec as P

F32 = jnp.float32
LANES = 128
PAD = 8
ROWS = 8
BASE = 8
EXT = 24
CROWS = 4
CBASE = 8
CEXT = 20
HALO = 6


def lanes_of(shape):
    return lax.broadcasted_iota(jnp.int32, shape, len(shape) - 1)


def spin(value, shift):
    return pltpu.roll(value, shift % LANES, 1)


def coef_tile(i, m, k_ref, r_ref, coefs, zs):
    diag, cx, cy, cz, cw = coefs
    y = PAD + 8 * m
    k = k_ref[i, y : y + 8, :]
    k_next = k_ref[i + 1, y : y + 8, :]
    k_prev = k_ref[i - 1, y : y + 8, :]
    lane = lanes_of(k.shape)
    x_next = 0.5 * (k + k_next)
    x_prev = 0.5 * (k + k_prev)
    y_next = 0.5 * (k + k_ref[i, y + 1 : y + 9, :])
    y_prev = 0.5 * (k + k_ref[i, y - 1 : y + 7, :])
    z_next = jnp.where(lane < LANES - zs, 0.5 * (k + spin(k, -zs)), 0.0)
    z_prev = jnp.where(lane >= zs, 0.5 * (k + spin(k, zs)), 0.0)
    edge = jnp.where((lane < zs) | (lane >= LANES - zs), 0.5 * k, 0.0)
    total = x_next + x_prev + y_next + y_prev + z_next + z_prev + edge
    diag[i, 8 * m : 8 * m + 8, :] = 1.0 + r_ref[i, y : y + 8, :] - total
    cx[i, 8 * m : 8 * m + 8, :] = jnp.where(jnp.minimum(k, k_next) > 0.0, x_next, 0.0)
    cy[i, y : y + 8, :] = y_next
    cz[i, 8 * m : 8 * m + 8, :] = z_next
    cw[i, 8 * m : 8 * m + 8, :] = z_prev


def blocks(count, unroll, block):
    if count <= unroll:
        block(0, count)
        return
    trips = -(-count // unroll)
    rows = -(-count // trips)
    whole = count // rows

    def body(j, carry):
        block(j * rows, rows)
        return carry

    lax.fori_loop(0, whole, body, 0)
    if count - whole * rows:
        block(whole * rows, count - whole * rows)


def build_coefs(k_ref, r_ref, coefs, lo, count, height, zs):
    _, cx, cy, _, _ = coefs
    for m in range(height // 8):
        y = PAD + 8 * m
        k = k_ref[lo - 1, y : y + 8, :]
        k_next = k_ref[lo, y : y + 8, :]
        cx[lo - 1, 8 * m : 8 * m + 8, :] = jnp.where(
            jnp.minimum(k, k_next) > 0.0, 0.5 * (k + k_next), 0.0
        )

    def block(first, rows):
        for i in range(rows):
            cy[lo + first + i, 0:PAD, :] = jnp.zeros((PAD, LANES), F32)
            for m in range(height // 8):
                coef_tile(lo + first + i, m, k_ref, r_ref, coefs, zs)

    blocks(count, 8 if height == 64 else 14, block)


def advance(src, dst, coefs, r_ref, lo, count, height, zs, windows, unroll=8):
    diag, cx, cy, cz, cw = coefs

    def block(first, rows):
        base = lo + first
        for m in range(height // 8):
            y = PAD + 8 * m
            here = slice(y, y + 8)
            tile = slice(8 * m, 8 * m + 8)
            line = [[src[w, base + i, here, :] for i in range(-1, rows + 1)] for w in range(windows)]
            across = [cx[base + i, tile, :] for i in range(-1, rows)]
            for i in range(rows):
                row = base + i
                a = diag[row, tile, :]
                r = r_ref[row, here, :]
                y_next, y_prev = cy[row, here, :], cy[row, y - 1 : y + 7, :]
                z_next, z_prev = cz[row, tile, :], cw[row, tile, :]
                for w in range(windows):
                    u = line[w][i + 1]
                    out = u * (a - r * (u * u))
                    out = out + (across[i + 1] * line[w][i + 2] + across[i] * line[w][i])
                    out = out + (y_next * src[w, row, y + 1 : y + 9, :] + y_prev * src[w, row, y - 1 : y + 7, :])
                    out = out + (z_next * spin(u, -zs) + z_prev * spin(u, zs))
                    dst[w, row, here, :] = out

    blocks(count, unroll, block)


def clear_pads(ref, lo, hi, height):
    zero = jnp.zeros((PAD, LANES), F32)

    def body(i, carry):
        for lead in range(ref.shape[0]):
            ref[lead, i, 0:PAD, :] = zero
            ref[lead, i, PAD + height : 2 * PAD + height, :] = zero
        return carry

    lax.fori_loop(lo, hi, body, 0)


def clear_pads_flat(ref, lo, hi, height):
    zero = jnp.zeros((PAD, LANES), F32)

    def body(i, carry):
        ref[i, 0:PAD, :] = zero
        ref[i, PAD + height : 2 * PAD + height, :] = zero
        return carry

    lax.fori_loop(lo, hi, body, 0)


def pair_lanes(e):
    even = lanes_of(e.shape) % 2 == 0
    return e + jnp.where(even, spin(e, -1), spin(e, 1))


def coarse_row(load):
    return 0.125 * pair_lanes((load(0, 0) + load(0, 1)) + (load(1, 0) + load(1, 1)))


def pack2(a, b):
    return jnp.where(lanes_of(a.shape) % 2 == 0, a, b)


def unpack_a(v):
    return jnp.where(lanes_of(v.shape) % 2 == 0, v, spin(v, 1))


def unpack_b(v):
    return jnp.where(lanes_of(v.shape) % 2 == 0, spin(v, -1), v)


def odd_here():
    return lax.axis_index("space") % 2


def pack_kernel(states, kappa, rate, send_out, send_in):
    odd = odd_here()
    out, near = 2 * odd, 2 - 2 * odd
    for i in range(HALO):
        for w in range(2):
            send_out[HALO * w + i] = states[w, out + i]
            send_in[HALO * w + i] = states[w, near + i]
        send_out[2 * HALO + i] = kappa[out + i]
        send_out[3 * HALO + i] = rate[out + i]
    for i in range(ROWS):
        send_in[2 * HALO + i] = kappa[i]
        send_in[2 * HALO + ROWS + i] = rate[i]


def place_halo(got, field, k_ext, r_ext, above, depth):
    for w in range(2):

        def halo(i, carry):
            field[w, 2 + 14 * above + i, PAD : PAD + 64, :] = got[HALO * w + i]
            return carry

        lax.fori_loop(0, HALO, halo, 0)
    low = 8 - depth

    def coef(i, carry):
        k_ext[low + (16 - low) * above + i, PAD : PAD + 64, :] = got[2 * HALO + i]
        r_ext[low + (16 - low) * above + i, PAD : PAD + 64, :] = got[2 * HALO + depth + i]
        return carry

    lax.fori_loop(0, depth, coef, 0)


def coarse_pair(k_ext, r_ext, fine):
    return pack2(
        coarse_row(lines_of(k_ext, (), fine)), 4.0 * coarse_row(lines_of(r_ext, (), fine))
    )


def place_own(states, field):
    def own(i, carry):
        for w in range(2):
            field[w, BASE + i, PAD : PAD + 64, :] = states[w, i]
        return carry

    lax.fori_loop(0, ROWS, own, 0)


def lines_of(ref, lead, row):
    return lambda part, first: ref[lead + (row + part, pl.ds(PAD + first, 32, stride=2))]


def inner_first_kernel(states, kappa, rate, got_in, late, field, other, diag, cx, cy, cz, cw, r_ext, k_ext):
    odd = odd_here()
    clear_pads_flat(k_ext, 0, EXT, 64)
    clear_pads(field, 0, EXT, 64)
    clear_pads(other, 0, EXT, 64)
    place_own(states, field)

    def own(i, carry):
        k_ext[BASE + i, PAD : PAD + 64, :] = kappa[i]
        r_ext[BASE + i, PAD : PAD + 64, :] = rate[i]
        return carry

    lax.fori_loop(0, ROWS, own, 0)
    place_halo(got_in, field, k_ext, r_ext, 1 - odd, ROWS)
    for i in range(2):
        late[i] = kappa[6 - 6 * odd + i]
        late[2 + i] = rate[6 - 6 * odd + i]
        late[4, 32 * i : 32 * i + 32, :] = coarse_pair(k_ext, r_ext, 16 - 12 * odd + 2 * i)
    coefs = (diag, cx, cy, cz, cw)
    build_coefs(k_ext, r_ext, coefs, 9 - 8 * odd, 14, 64, 1)
    src, dst = field, other
    for n in range(1, 7):
        advance(src, dst, coefs, r_ext, BASE + n - 6 * odd, 14 - 2 * n, 64, 1, 2)
        src, dst = dst, src


def outer_first_kernel(got_out, *refs):
    refs = refs[9:]
    send_out, send_in, field, other, diag, cx, cy, cz, cw, r_ext, k_ext = refs
    odd = odd_here()
    place_halo(got_out, field, k_ext, r_ext, odd, HALO)
    coefs = (diag, cx, cy, cz, cw)
    build_coefs(k_ext, r_ext, coefs, 3 + 12 * odd, 6, 64, 1)
    src, dst = field, other
    for n in range(1, 7):
        advance(src, dst, coefs, r_ext, 2 + n + (14 - 2 * n) * odd, 6, 64, 1, 2)
        src, dst = dst, src

    def own(i, carry):
        for w in range(2):
            value = src[w, BASE + i, PAD : PAD + 64, :]
            send_out[ROWS * w + i] = value
            send_in[ROWS * w + i] = value
        return carry

    lax.fori_loop(0, ROWS, own, 0)
    for i in range(2):
        send_in[16, 32 * i : 32 * i + 32, :] = coarse_pair(k_ext, r_ext, 4 + 12 * odd + 2 * i)


def inner_second_kernel(got_in, got_late, *refs):
    refs = refs[9:]
    field, other, diag, cx, cy, cz, cw, r_ext, k_ext = refs
    odd = odd_here()

    def halo(i, carry):
        for w in range(2):
            field[w, 16 - 16 * odd + i, PAD : PAD + 64, :] = got_in[ROWS * w + i]
        return carry

    lax.fori_loop(0, ROWS, halo, 0)
    for i in range(2):
        k_ext[22 * odd + i, PAD : PAD + 64, :] = got_late[i]
        r_ext[22 * odd + i, PAD : PAD + 64, :] = got_late[2 + i]
    coefs = (diag, cx, cy, cz, cw)
    build_coefs(k_ext, r_ext, coefs, 1 + 20 * odd, 2, 64, 1)
    src, dst = field, other
    for n in range(1, 7):
        advance(src, dst, coefs, r_ext, BASE + n - 8 * odd, 16 - 2 * n, 64, 1, 2)
        src, dst = dst, src


def outer_second_kernel(got_out, *refs):
    _, _, diag, cx, cy, cz, cw, r_ext, old, field, other, send = refs
    odd = odd_here()

    def halo(i, carry):
        for w in range(2):
            field[w, 16 * odd + i, PAD : PAD + 64, :] = got_out[ROWS * w + i]
        return carry

    lax.fori_loop(0, ROWS, halo, 0)
    coefs = (diag, cx, cy, cz, cw)
    src, dst = field, other
    for n in range(1, 7):
        advance(src, dst, coefs, r_ext, n + (16 - 2 * n) * odd, 8, 64, 1, 2)
        src, dst = dst, src
    later = (lax.axis_index("tm") > 0).astype(F32)
    for i in range(-1, 5):
        rows = []
        for w in range(2):
            value = coarse_row(lines_of(src, (w,), BASE + 2 * i))
            if 0 <= i < CROWS:
                value = value - (old[w, i] if w else later * old[w, i])
            rows.append(value)
        send[1 + i] = pack2(*rows)


def old_kernel(states, got_out, got_in, k_ext, r_ext, old, kc, rc, field, diag, cx, cy, cz, cw, here, there):
    odd = odd_here()
    place_own(states, field)
    for got, above in ((got_out, odd), (got_in, 1 - odd)):
        for w in range(2):

            def halo(i, carry):
                field[w, 2 + 14 * above + i, PAD : PAD + 64, :] = got[HALO * w + i]
                return carry

            lax.fori_loop(0, HALO, halo, 0)
    clear_pads_flat(kc, 0, CEXT, 32)
    clear_pads(here, 0, CEXT, 32)
    clear_pads(there, 0, CEXT, 32)

    def row_coefs(first, rows):
        for i in range(rows):
            at = first + i
            kc[CBASE - 4 + at, PAD : PAD + 32, :] = coarse_row(lines_of(k_ext, (), 2 * at))
            rc[CBASE - 4 + at, PAD : PAD + 32, :] = 4.0 * coarse_row(lines_of(r_ext, (), 2 * at))

    blocks(12, 6, row_coefs)

    def row_states(first, rows):
        for i in range(rows):
            for w in range(2):
                value = coarse_row(lines_of(field, (w,), 2 + 2 * (first + i)))
                here[w, CBASE - 3 + first + i, PAD : PAD + 32, :] = value

    blocks(10, 5, row_states)
    coefs = (diag, cx, cy, cz, cw)
    build_coefs(kc, rc, coefs, CBASE - 2, CROWS + 4, 32, 2)
    src, dst = here, there
    for n in range(3):
        reach = 2 - n
        advance(src, dst, coefs, rc, CBASE - reach, CROWS + 2 * reach, 32, 2, 2)
        src, dst = dst, src
    for w in range(2):
        for i in range(CROWS):
            old[w, i] = src[w, CBASE + i, PAD : PAD + 32, :]


def chain_coefs_kernel(kc_near, rc_near, got_late, got_in2, rc, diag, cx, cy, cz, cw, kc):
    odd = odd_here()
    clear_pads_flat(kc, 0, CEXT, 32)

    def near(i, carry):
        kc[i, PAD : PAD + 32, :] = kc_near[i, PAD : PAD + 32, :]
        rc[i, PAD : PAD + 32, :] = rc_near[i, PAD : PAD + 32, :]
        return carry

    lax.fori_loop(CBASE - 4, CBASE + 8, near, 0)
    for got, slot, above in ((got_late, 4, odd), (got_in2, 16, 1 - odd)):
        for j in range(2):
            packed = got[slot, 32 * j : 32 * j + 32, :]
            row = CBASE - 6 + 14 * above + j
            kc[row, PAD : PAD + 32, :] = unpack_a(packed)
            rc[row, PAD : PAD + 32, :] = unpack_b(packed)
    build_coefs(kc, rc, (diag, cx, cy, cz, cw), CBASE - 5, CROWS + 10, 32, 2)


def third_kernel(
    sent, got_out, got_in, rc, diag, cx, cy, cz, cw,
    tm_mid, tm_up, tm_down, first, newer, here, there,
):
    odd = odd_here()
    clear_pads(here, 0, CEXT, 32)
    clear_pads(there, 0, CEXT, 32)
    coefs = (diag, cx, cy, cz, cw)
    for i in range(CROWS):
        here[0, CBASE + i, PAD : PAD + 32, :] = unpack_a(sent[1 + i])
        there[1, CBASE + i, PAD : PAD + 32, :] = unpack_b(sent[1 + i])
    for got, above in ((got_out, odd), (got_in, 1 - odd)):
        for j in range(5):
            packed = got[above + j]
            row = CBASE - 5 + 9 * above + j
            here[0, row, PAD : PAD + 32, :] = unpack_a(packed)
            there[1, row, PAD : PAD + 32, :] = unpack_b(packed)
    for i in range(-3, 7):
        first[3 + i] = here[0, CBASE + i, PAD : PAD + 32, :]
    advance(here, there, coefs, rc, CBASE - 4, CROWS + 8, 32, 2, 1, 14)
    advance(there, here, coefs, rc, CBASE - 3, CROWS + 6, 32, 2, 1, 14)
    advance(here, there, coefs, rc, CBASE - 2, CROWS + 4, 32, 2, 1, 14)
    carried = []
    for i in range(-2, 6):
        moved = there[0, CBASE + i, PAD : PAD + 32, :]
        if 0 <= i < CROWS:
            newer[i] = moved
        carried.append(moved + there[1, CBASE + i, PAD : PAD + 32, :])
    for j in range(4):
        tm_mid[j] = pack2(carried[2 * j], carried[2 * j + 1])
    for j in range(2):
        tm_up[j] = pack2(carried[2 * j], carried[2 * j + 1])
        tm_down[j] = pack2(carried[4 + 2 * j], carried[5 + 2 * j])


def last_kernel(
    fine, old, first, newer, tm_mid, from_below, from_above, rc, diag, cx, cy, cz, cw, ends, here, there
):
    clear_pads(here, 0, CEXT, 32)
    clear_pads(there, 0, CEXT, 32)
    for ref, start, count in ((from_below, -6, 2), (tm_mid, -2, 4), (from_above, 6, 2)):
        for j in range(count):
            row = CBASE + start + 2 * j
            here[0, row, PAD : PAD + 32, :] = unpack_a(ref[j])
            here[0, row + 1, PAD : PAD + 32, :] = unpack_b(ref[j])
    coefs = (diag, cx, cy, cz, cw)
    advance(here, there, coefs, rc, CBASE - 5, CROWS + 10, 32, 2, 1, 14)
    advance(there, here, coefs, rc, CBASE - 4, CROWS + 8, 32, 2, 1, 14)
    advance(here, there, coefs, rc, CBASE - 3, CROWS + 6, 32, 2, 1, 14)
    second = []
    for i in range(-3, 7):
        moved = there[0, CBASE + i, PAD : PAD + 32, :]
        if 0 <= i < CROWS:
            second.append(moved)
        here[0, CBASE + i, PAD : PAD + 32, :] = first[3 + i] + moved
    advance(here, there, coefs, rc, CBASE - 2, CROWS + 4, 32, 2, 1, 14)
    advance(there, here, coefs, rc, CBASE - 1, CROWS + 2, 32, 2, 1, 14)
    advance(here, there, coefs, rc, CBASE, CROWS, 32, 2, 1, 14)
    later = lax.axis_index("tm") > 0
    for i in range(CROWS):
        third = there[0, CBASE + i, PAD : PAD + 32, :]
        shifts = (
            jnp.where(later, second[i] - old[0, i], 0.0),
            jnp.where(later, third, newer[i]) - old[1, i],
        )
        for w in range(2):
            for part in range(2):
                for line in range(2):
                    value = fine[w, BASE + 2 * i + part, pl.ds(PAD + line, 32, stride=2), :]
                    ends[w, 2 * i + part, pl.ds(line, 32, stride=2), :] = value + shifts[w]


def shape(*sizes):
    return jax.ShapeDtypeStruct(sizes, F32)


def call(kernel, outs, scratch, cost, *args, aliases=None):
    return pl.pallas_call(
        kernel,
        out_shape=outs,
        in_specs=[pl.BlockSpec(memory_space=pltpu.VMEM)] * len(args),
        out_specs=[pl.BlockSpec(memory_space=pltpu.VMEM)] * len(outs),
        scratch_shapes=[pltpu.VMEM(sizes, F32) for sizes in scratch],
        input_output_aliases=aliases or {},
        compiler_params=pltpu.CompilerParams(vmem_limit_bytes=24 * 1024 * 1024),
        cost_estimate=pl.CostEstimate(flops=cost, bytes_accessed=1 << 20, transcendentals=0),
    )(*args)


def swap(value, odd_pairs):
    count, groups = lax.axis_size("space"), lax.axis_size("tm")
    pairs = []
    for group in range(groups):
        for low in range(1 if odd_pairs else 0, count - 1, 2):
            a, b = group * count + low, group * count + low + 1
            pairs += [(a, b), (b, a)]
    return lax.ppermute(value, ("tm", "space"), pairs)


def over_tm(value, offset):
    count = lax.axis_size("space")
    pairs = [(s, count + s + offset) for s in range(count) if 0 <= s + offset < count]
    return lax.ppermute(value, ("tm", "space"), pairs)


FINE_COEFS = [(EXT, 64, LANES), (EXT, 64, LANES), (EXT, 64 + 2 * PAD, LANES), (EXT, 64, LANES), (EXT, 64, LANES)]
COARSE_COEFS = [(CEXT, 32, LANES), (CEXT, 32, LANES), (CEXT, 32 + 2 * PAD, LANES), (CEXT, 32, LANES), (CEXT, 32, LANES)]
FINE_FIELD = (2, EXT, 64 + 2 * PAD, LANES)
FINE_FLAT = (EXT, 64 + 2 * PAD, LANES)
COARSE_FIELD = (2, CEXT, 32 + 2 * PAD, LANES)
COARSE_FLAT = (CEXT, 32 + 2 * PAD, LANES)


def swaps(value_out, value_in):
    got_out = swap(value_out, True)
    got_in = swap(value_in, False)
    return got_out, got_in


COST = 10_000_000


def shards(states, kappa, rate):
    fields = [shape(*FINE_FIELD)] * 2
    fine_coefs = [shape(*sizes) for sizes in FINE_COEFS]
    coarse_coefs = [shape(*sizes) for sizes in COARSE_COEFS]
    send_out, send_in = call(
        pack_kernel, [shape(4 * HALO, 64, LANES), shape(2 * HALO + 2 * ROWS, 64, LANES)],
        [], 1000, states, kappa, rate,
    )
    got_out, got_in = swaps(send_out, send_in)
    late, *work = call(
        inner_first_kernel,
        [shape(5, 64, LANES)] + fields + fine_coefs + [shape(*FINE_FLAT)] * 2,
        [], COST, states, kappa, rate, got_in,
    )
    got_late = swap(late, True)
    send_out2, send_in2, *work = call(
        outer_first_kernel,
        [shape(16, 64, LANES), shape(17, 64, LANES)] + fields + fine_coefs + [shape(*FINE_FLAT)] * 2,
        [], COST, got_out, *work, aliases={1 + n: 2 + n for n in range(9)},
    )
    got_out2, got_in2 = swaps(send_out2, send_in2)
    field, other, *coefs, r_ext, k_ext = call(
        inner_second_kernel, fields + fine_coefs + [shape(*FINE_FLAT)] * 2,
        [], COST, got_in2, got_late, *work, aliases={2 + n: n for n in range(9)},
    )
    old, kc, rc = call(
        old_kernel,
        [shape(2, CROWS, 32, LANES), shape(*COARSE_FLAT), shape(*COARSE_FLAT)],
        [FINE_FIELD] + COARSE_COEFS + [COARSE_FIELD] * 2,
        COST, states, got_out, got_in, k_ext, r_ext,
    )
    field, other, send3 = call(
        outer_second_kernel,
        fields + [shape(6, 32, LANES)],
        [], COST, got_out2, field, other, *coefs, r_ext, old, aliases={1: 0, 2: 1},
    )
    got_out3, got_in3 = swaps(send3, send3)
    rc2, *coarse = call(
        chain_coefs_kernel, [shape(*COARSE_FLAT)] + coarse_coefs, [COARSE_FLAT],
        COST, kc, rc, got_late, got_in2,
    )
    tm_mid, tm_up, tm_down, first, newer = call(
        third_kernel,
        [shape(4, 32, LANES), shape(2, 32, LANES), shape(2, 32, LANES), shape(10, 32, LANES), shape(CROWS, 32, LANES)],
        [COARSE_FIELD] * 2,
        COST, send3, got_out3, got_in3, rc2, *coarse,
    )
    from_below = over_tm(tm_up, 1)
    from_above = over_tm(tm_down, -1)
    mid = over_tm(tm_mid, 0)
    (ends,) = call(
        last_kernel,
        [shape(2, ROWS, 64, LANES)],
        [COARSE_FIELD] * 2,
        COST, field, old, first, newer, mid, from_below, from_above, rc2, *coarse,
    )
    return ends


def solution(mesh):
    in_specs = (P("tm", "space", None, None), P("space", None, None), P("space", None, None))
    out_specs = P("tm", "space", None, None)
    return jax.shard_map(shards, mesh=mesh, in_specs=in_specs, out_specs=out_specs, check_vma=False)
```

```python
import jax
import jax.numpy as jnp
from jax import lax
from jax.experimental import pallas as pl
from jax.experimental.pallas import tpu as pltpu
from jax.sharding import PartitionSpec as P

F32 = jnp.float32
LANES = 128
PAD = 8
ROWS = 8
BASE = 8
EXT = 24
CROWS = 4
CBASE = 8
CEXT = 20
HALO = 6


def lanes_of(shape):
    return lax.broadcasted_iota(jnp.int32, shape, len(shape) - 1)


def spin(value, shift):
    return pltpu.roll(value, shift % LANES, 1)


def coef_tile(i, m, k_ref, r_ref, coefs, zs):
    diag, cx, cy, cz, cw = coefs
    y = PAD + 8 * m
    k = k_ref[i, y : y + 8, :]
    k_next = k_ref[i + 1, y : y + 8, :]
    k_prev = k_ref[i - 1, y : y + 8, :]
    lane = lanes_of(k.shape)
    x_next = 0.5 * (k + k_next)
    x_prev = 0.5 * (k + k_prev)
    y_next = 0.5 * (k + k_ref[i, y + 1 : y + 9, :])
    y_prev = 0.5 * (k + k_ref[i, y - 1 : y + 7, :])
    z_next = jnp.where(lane < LANES - zs, 0.5 * (k + spin(k, -zs)), 0.0)
    z_prev = jnp.where(lane >= zs, 0.5 * (k + spin(k, zs)), 0.0)
    edge = jnp.where((lane < zs) | (lane >= LANES - zs), 0.5 * k, 0.0)
    total = x_next + x_prev + y_next + y_prev + z_next + z_prev + edge
    diag[i, 8 * m : 8 * m + 8, :] = 1.0 + r_ref[i, y : y + 8, :] - total
    cx[i, 8 * m : 8 * m + 8, :] = jnp.where(jnp.minimum(k, k_next) > 0.0, x_next, 0.0)
    cy[i, y : y + 8, :] = y_next
    cz[i, 8 * m : 8 * m + 8, :] = z_next
    cw[i, 8 * m : 8 * m + 8, :] = z_prev


def blocks(count, unroll, block):
    if count <= unroll:
        block(0, count)
        return
    trips = -(-count // unroll)
    rows = -(-count // trips)
    whole = count // rows

    def body(j, carry):
        block(j * rows, rows)
        return carry

    lax.fori_loop(0, whole, body, 0)
    if count - whole * rows:
        block(whole * rows, count - whole * rows)


def build_coefs(k_ref, r_ref, coefs, lo, count, height, zs):
    _, cx, cy, _, _ = coefs
    for m in range(height // 8):
        y = PAD + 8 * m
        k = k_ref[lo - 1, y : y + 8, :]
        k_next = k_ref[lo, y : y + 8, :]
        cx[lo - 1, 8 * m : 8 * m + 8, :] = jnp.where(
            jnp.minimum(k, k_next) > 0.0, 0.5 * (k + k_next), 0.0
        )

    def block(first, rows):
        for i in range(rows):
            cy[lo + first + i, 0:PAD, :] = jnp.zeros((PAD, LANES), F32)
            for m in range(height // 8):
                coef_tile(lo + first + i, m, k_ref, r_ref, coefs, zs)

    blocks(count, 8 if height == 64 else 14, block)


def advance(src, dst, coefs, r_ref, lo, count, height, zs, windows, unroll=8):
    diag, cx, cy, cz, cw = coefs

    def block(first, rows):
        base = lo + first
        for m in range(height // 8):
            y = PAD + 8 * m
            here = slice(y, y + 8)
            tile = slice(8 * m, 8 * m + 8)
            line = [[src[w, base + i, here, :] for i in range(-1, rows + 1)] for w in range(windows)]
            across = [cx[base + i, tile, :] for i in range(-1, rows)]
            for i in range(rows):
                row = base + i
                a = diag[row, tile, :]
                r = r_ref[row, here, :]
                y_next, y_prev = cy[row, here, :], cy[row, y - 1 : y + 7, :]
                z_next, z_prev = cz[row, tile, :], cw[row, tile, :]
                for w in range(windows):
                    u = line[w][i + 1]
                    out = u * (a - r * (u * u))
                    out = out + (across[i + 1] * line[w][i + 2] + across[i] * line[w][i])
                    out = out + (y_next * src[w, row, y + 1 : y + 9, :] + y_prev * src[w, row, y - 1 : y + 7, :])
                    out = out + (z_next * spin(u, -zs) + z_prev * spin(u, zs))
                    dst[w, row, here, :] = out

    blocks(count, unroll, block)


def clear_pads(ref, lo, hi, height):
    zero = jnp.zeros((PAD, LANES), F32)

    def body(i, carry):
        for lead in range(ref.shape[0]):
            ref[lead, i, 0:PAD, :] = zero
            ref[lead, i, PAD + height : 2 * PAD + height, :] = zero
        return carry

    lax.fori_loop(lo, hi, body, 0)


def clear_pads_flat(ref, lo, hi, height):
    zero = jnp.zeros((PAD, LANES), F32)

    def body(i, carry):
        ref[i, 0:PAD, :] = zero
        ref[i, PAD + height : 2 * PAD + height, :] = zero
        return carry

    lax.fori_loop(lo, hi, body, 0)


def pair_lanes(e):
    even = lanes_of(e.shape) % 2 == 0
    return e + jnp.where(even, spin(e, -1), spin(e, 1))


def coarse_row(load):
    return 0.125 * pair_lanes((load(0, 0) + load(0, 1)) + (load(1, 0) + load(1, 1)))


def pack2(a, b):
    return jnp.where(lanes_of(a.shape) % 2 == 0, a, b)


def unpack_a(v):
    return jnp.where(lanes_of(v.shape) % 2 == 0, v, spin(v, 1))


def unpack_b(v):
    return jnp.where(lanes_of(v.shape) % 2 == 0, spin(v, -1), v)


def odd_here():
    return lax.axis_index("space") % 2


def pack_kernel(states, kappa, rate, send_out, send_in):
    odd = odd_here()
    out, near = 2 * odd, 2 - 2 * odd
    for i in range(HALO):
        for w in range(2):
            send_out[HALO * w + i] = states[w, out + i]
            send_in[HALO * w + i] = states[w, near + i]
        send_out[2 * HALO + i] = kappa[out + i]
        send_out[3 * HALO + i] = rate[out + i]
    for i in range(ROWS):
        send_in[2 * HALO + i] = kappa[i]
        send_in[2 * HALO + ROWS + i] = rate[i]


def place_halo(got, field, k_ext, r_ext, above, depth):
    for w in range(2):

        def halo(i, carry):
            field[w, 2 + 14 * above + i, PAD : PAD + 64, :] = got[HALO * w + i]
            return carry

        lax.fori_loop(0, HALO, halo, 0)
    low = 8 - depth

    def coef(i, carry):
        k_ext[low + (16 - low) * above + i, PAD : PAD + 64, :] = got[2 * HALO + i]
        r_ext[low + (16 - low) * above + i, PAD : PAD + 64, :] = got[2 * HALO + depth + i]
        return carry

    lax.fori_loop(0, depth, coef, 0)


def coarse_pair(k_ext, r_ext, fine):
    return pack2(
        coarse_row(lines_of(k_ext, (), fine)), 4.0 * coarse_row(lines_of(r_ext, (), fine))
    )


def place_own(states, field):
    def own(i, carry):
        for w in range(2):
            field[w, BASE + i, PAD : PAD + 64, :] = states[w, i]
        return carry

    lax.fori_loop(0, ROWS, own, 0)


def lines_of(ref, lead, row):
    return lambda part, first: ref[lead + (row + part, pl.ds(PAD + first, 32, stride=2))]


def inner_first_kernel(states, kappa, rate, got_in, late, field, other, diag, cx, cy, cz, cw, r_ext, k_ext):
    odd = odd_here()
    clear_pads_flat(k_ext, 0, EXT, 64)
    clear_pads(field, 0, EXT, 64)
    clear_pads(other, 0, EXT, 64)
    place_own(states, field)

    def own(i, carry):
        k_ext[BASE + i, PAD : PAD + 64, :] = kappa[i]
        r_ext[BASE + i, PAD : PAD + 64, :] = rate[i]
        return carry

    lax.fori_loop(0, ROWS, own, 0)
    place_halo(got_in, field, k_ext, r_ext, 1 - odd, ROWS)
    for i in range(2):
        late[i] = kappa[6 - 6 * odd + i]
        late[2 + i] = rate[6 - 6 * odd + i]
        late[4, 32 * i : 32 * i + 32, :] = coarse_pair(k_ext, r_ext, 16 - 12 * odd + 2 * i)
    coefs = (diag, cx, cy, cz, cw)
    build_coefs(k_ext, r_ext, coefs, 9 - 8 * odd, 14, 64, 1)
    src, dst = field, other
    for n in range(1, 7):
        advance(src, dst, coefs, r_ext, BASE + n - 6 * odd, 14 - 2 * n, 64, 1, 2)
        src, dst = dst, src


def outer_first_kernel(got_out, *refs):
    refs = refs[9:]
    send_out, send_in, field, other, diag, cx, cy, cz, cw, r_ext, k_ext = refs
    odd = odd_here()
    place_halo(got_out, field, k_ext, r_ext, odd, HALO)
    coefs = (diag, cx, cy, cz, cw)
    build_coefs(k_ext, r_ext, coefs, 3 + 12 * odd, 6, 64, 1)
    src, dst = field, other
    for n in range(1, 7):
        advance(src, dst, coefs, r_ext, 2 + n + (14 - 2 * n) * odd, 6, 64, 1, 2)
        src, dst = dst, src

    def own(i, carry):
        for w in range(2):
            send_in[ROWS * w + i] = src[w, BASE + i, PAD : PAD + 64, :]
        send_out[i] = src[0, BASE + i, PAD : PAD + 64, :]
        return carry

    lax.fori_loop(0, ROWS, own, 0)

    def near(i, carry):
        send_out[ROWS + i] = src[1, BASE + 2 * odd + i, PAD : PAD + 64, :]
        return carry

    lax.fori_loop(0, HALO, near, 0)
    for i in range(2):
        send_in[16, 32 * i : 32 * i + 32, :] = coarse_pair(k_ext, r_ext, 4 + 12 * odd + 2 * i)


def inner_second_kernel(got_in, got_late, *refs):
    refs = refs[9:]
    field, other, diag, cx, cy, cz, cw, r_ext, k_ext = refs
    odd = odd_here()

    def halo(i, carry):
        for w in range(2):
            field[w, 16 - 16 * odd + i, PAD : PAD + 64, :] = got_in[ROWS * w + i]
        return carry

    lax.fori_loop(0, ROWS, halo, 0)
    for i in range(2):
        k_ext[22 * odd + i, PAD : PAD + 64, :] = got_late[i]
        r_ext[22 * odd + i, PAD : PAD + 64, :] = got_late[2 + i]
    coefs = (diag, cx, cy, cz, cw)
    build_coefs(k_ext, r_ext, coefs, 1 + 20 * odd, 2, 64, 1)
    src, dst = field, other
    for n in range(1, 7):
        advance(src, dst, coefs, r_ext, BASE + n - 8 * odd, 16 - 2 * n, 64, 1, 2)
        src, dst = dst, src


def outer_second_kernel(got_out, *refs):
    _, _, diag, cx, cy, cz, cw, r_ext, old, field, other, send = refs
    odd = odd_here()

    def halo(i, carry):
        field[0, 16 * odd + i, PAD : PAD + 64, :] = got_out[i]
        return carry

    def near(i, carry):
        field[1, 2 + 14 * odd + i, PAD : PAD + 64, :] = got_out[ROWS + i]
        return carry

    lax.fori_loop(0, ROWS, halo, 0)
    lax.fori_loop(0, HALO, near, 0)
    for i in range(2):
        field[1, 22 * odd + i, PAD : PAD + 64, :] = jnp.zeros((64, LANES), F32)
    coefs = (diag, cx, cy, cz, cw)
    src, dst = field, other
    for n in range(1, 7):
        advance(src, dst, coefs, r_ext, n + (16 - 2 * n) * odd, 8, 64, 1, 2)
        src, dst = dst, src
    later = (lax.axis_index("tm") > 0).astype(F32)
    for i in range(-1, 5):
        rows = []
        for w in range(2):
            value = coarse_row(lines_of(src, (w,), BASE + 2 * i))
            if 0 <= i < CROWS:
                value = value - (old[w, i] if w else later * old[w, i])
            rows.append(value)
        send[1 + i] = pack2(*rows)


def old_kernel(states, got_out, got_in, k_ext, r_ext, old, kc, rc, field, diag, cx, cy, cz, cw, here, there):
    odd = odd_here()
    place_own(states, field)
    for got, above in ((got_out, odd), (got_in, 1 - odd)):
        for w in range(2):

            def halo(i, carry):
                field[w, 2 + 14 * above + i, PAD : PAD + 64, :] = got[HALO * w + i]
                return carry

            lax.fori_loop(0, HALO, halo, 0)
    clear_pads_flat(kc, 0, CEXT, 32)
    clear_pads(here, 0, CEXT, 32)
    clear_pads(there, 0, CEXT, 32)

    def row_coefs(first, rows):
        for i in range(rows):
            at = first + i
            kc[CBASE - 4 + at, PAD : PAD + 32, :] = coarse_row(lines_of(k_ext, (), 2 * at))
            rc[CBASE - 4 + at, PAD : PAD + 32, :] = 4.0 * coarse_row(lines_of(r_ext, (), 2 * at))

    blocks(12, 6, row_coefs)

    def row_states(first, rows):
        for i in range(rows):
            for w in range(2):
                value = coarse_row(lines_of(field, (w,), 2 + 2 * (first + i)))
                here[w, CBASE - 3 + first + i, PAD : PAD + 32, :] = value

    blocks(10, 5, row_states)
    coefs = (diag, cx, cy, cz, cw)
    build_coefs(kc, rc, coefs, CBASE - 2, CROWS + 4, 32, 2)
    src, dst = here, there
    for n in range(3):
        reach = 2 - n
        advance(src, dst, coefs, rc, CBASE - reach, CROWS + 2 * reach, 32, 2, 2)
        src, dst = dst, src
    for w in range(2):
        for i in range(CROWS):
            old[w, i] = src[w, CBASE + i, PAD : PAD + 32, :]


def chain_coefs_kernel(kc_near, rc_near, got_late, got_in2, rc, diag, cx, cy, cz, cw, kc):
    odd = odd_here()
    clear_pads_flat(kc, 0, CEXT, 32)

    def near(i, carry):
        kc[i, PAD : PAD + 32, :] = kc_near[i, PAD : PAD + 32, :]
        rc[i, PAD : PAD + 32, :] = rc_near[i, PAD : PAD + 32, :]
        return carry

    lax.fori_loop(CBASE - 4, CBASE + 8, near, 0)
    for got, slot, above in ((got_late, 4, odd), (got_in2, 16, 1 - odd)):
        for j in range(2):
            packed = got[slot, 32 * j : 32 * j + 32, :]
            row = CBASE - 6 + 14 * above + j
            kc[row, PAD : PAD + 32, :] = unpack_a(packed)
            rc[row, PAD : PAD + 32, :] = unpack_b(packed)
    build_coefs(kc, rc, (diag, cx, cy, cz, cw), CBASE - 5, CROWS + 10, 32, 2)


def third_kernel(
    sent, got_out, got_in, rc, diag, cx, cy, cz, cw,
    tm_mid, tm_out, tm_in, first, newer, here, there,
):
    odd = odd_here()
    clear_pads(here, 0, CEXT, 32)
    clear_pads(there, 0, CEXT, 32)
    coefs = (diag, cx, cy, cz, cw)
    for i in range(CROWS):
        here[0, CBASE + i, PAD : PAD + 32, :] = unpack_a(sent[1 + i])
        there[1, CBASE + i, PAD : PAD + 32, :] = unpack_b(sent[1 + i])
    for got, above in ((got_out, odd), (got_in, 1 - odd)):
        for j in range(5):
            packed = got[above + j]
            row = CBASE - 5 + 9 * above + j
            here[0, row, PAD : PAD + 32, :] = unpack_a(packed)
            there[1, row, PAD : PAD + 32, :] = unpack_b(packed)
    for i in range(-3, 7):
        first[3 + i] = here[0, CBASE + i, PAD : PAD + 32, :]
    advance(here, there, coefs, rc, CBASE - 4, CROWS + 8, 32, 2, 1, 14)
    advance(there, here, coefs, rc, CBASE - 3, CROWS + 6, 32, 2, 1, 14)
    advance(here, there, coefs, rc, CBASE - 2, CROWS + 4, 32, 2, 1, 14)
    carried = []
    for i in range(-2, 6):
        moved = there[0, CBASE + i, PAD : PAD + 32, :]
        if 0 <= i < CROWS:
            newer[i] = moved
        carried.append(moved + there[1, CBASE + i, PAD : PAD + 32, :])
    for j in range(4):
        tm_mid[j] = pack2(carried[2 * j], carried[2 * j + 1])
    for j in range(2):
        low = pack2(carried[2 * j], carried[2 * j + 1])
        high = pack2(carried[4 + 2 * j], carried[5 + 2 * j])
        tm_out[j] = jnp.where(odd > 0, low, high)
        tm_in[j] = jnp.where(odd > 0, high, low)


def last_kernel(
    fine, old, first, newer, tm_mid, from_out, from_in, rc, diag, cx, cy, cz, cw, ends, here, there
):
    clear_pads(here, 0, CEXT, 32)
    clear_pads(there, 0, CEXT, 32)
    odd = odd_here()
    for ref, start, count in ((from_out, 12 * odd - 6, 2), (tm_mid, -2, 4), (from_in, 6 - 12 * odd, 2)):
        for j in range(count):
            row = CBASE + start + 2 * j
            here[0, row, PAD : PAD + 32, :] = unpack_a(ref[j])
            here[0, row + 1, PAD : PAD + 32, :] = unpack_b(ref[j])
    coefs = (diag, cx, cy, cz, cw)
    advance(here, there, coefs, rc, CBASE - 5, CROWS + 10, 32, 2, 1, 14)
    advance(there, here, coefs, rc, CBASE - 4, CROWS + 8, 32, 2, 1, 14)
    advance(here, there, coefs, rc, CBASE - 3, CROWS + 6, 32, 2, 1, 14)
    second = []
    for i in range(-3, 7):
        moved = there[0, CBASE + i, PAD : PAD + 32, :]
        if 0 <= i < CROWS:
            second.append(moved)
        here[0, CBASE + i, PAD : PAD + 32, :] = first[3 + i] + moved
    advance(here, there, coefs, rc, CBASE - 2, CROWS + 4, 32, 2, 1, 14)
    advance(there, here, coefs, rc, CBASE - 1, CROWS + 2, 32, 2, 1, 14)
    advance(here, there, coefs, rc, CBASE, CROWS, 32, 2, 1, 14)
    later = lax.axis_index("tm") > 0
    for i in range(CROWS):
        third = there[0, CBASE + i, PAD : PAD + 32, :]
        shifts = (
            jnp.where(later, second[i] - old[0, i], 0.0),
            jnp.where(later, third, newer[i]) - old[1, i],
        )
        for w in range(2):
            for part in range(2):
                for line in range(2):
                    value = fine[w, BASE + 2 * i + part, pl.ds(PAD + line, 32, stride=2), :]
                    ends[w, 2 * i + part, pl.ds(line, 32, stride=2), :] = value + shifts[w]


def shape(*sizes):
    return jax.ShapeDtypeStruct(sizes, F32)


def call(kernel, outs, scratch, cost, *args, aliases=None):
    return pl.pallas_call(
        kernel,
        out_shape=outs,
        in_specs=[pl.BlockSpec(memory_space=pltpu.VMEM)] * len(args),
        out_specs=[pl.BlockSpec(memory_space=pltpu.VMEM)] * len(outs),
        scratch_shapes=[pltpu.VMEM(sizes, F32) for sizes in scratch],
        input_output_aliases=aliases or {},
        compiler_params=pltpu.CompilerParams(vmem_limit_bytes=24 * 1024 * 1024),
        cost_estimate=pl.CostEstimate(flops=cost, bytes_accessed=1 << 20, transcendentals=0),
    )(*args)


def partners(odd_pairs):
    count = lax.axis_size("space")
    lows = range(1 if odd_pairs else 0, count - 1, 2)
    return [pair for low in lows for pair in ((low, low + 1), (low + 1, low))]


def swap(value, odd_pairs):
    count = lax.axis_size("space")
    starts = [group * count for group in range(lax.axis_size("tm"))]
    pairs = [(start + a, start + b) for start in starts for a, b in partners(odd_pairs)]
    return lax.ppermute(value, ("tm", "space"), pairs)


def over_tm(value, odd_pairs):
    count = lax.axis_size("space")
    pairs = [(s, s) for s in range(count)] if odd_pairs is None else partners(odd_pairs)
    return lax.ppermute(value, ("tm", "space"), [(a, count + b) for a, b in pairs])


FINE_COEFS = [(EXT, 64, LANES), (EXT, 64, LANES), (EXT, 64 + 2 * PAD, LANES), (EXT, 64, LANES), (EXT, 64, LANES)]
COARSE_COEFS = [(CEXT, 32, LANES), (CEXT, 32, LANES), (CEXT, 32 + 2 * PAD, LANES), (CEXT, 32, LANES), (CEXT, 32, LANES)]
FINE_FIELD = (2, EXT, 64 + 2 * PAD, LANES)
FINE_FLAT = (EXT, 64 + 2 * PAD, LANES)
COARSE_FIELD = (2, CEXT, 32 + 2 * PAD, LANES)
COARSE_FLAT = (CEXT, 32 + 2 * PAD, LANES)


def swaps(value_out, value_in):
    got_out = swap(value_out, True)
    got_in = swap(value_in, False)
    return got_out, got_in


COST = 10_000_000


def shards(states, kappa, rate):
    fields = [shape(*FINE_FIELD)] * 2
    fine_coefs = [shape(*sizes) for sizes in FINE_COEFS]
    coarse_coefs = [shape(*sizes) for sizes in COARSE_COEFS]
    send_out, send_in = call(
        pack_kernel, [shape(4 * HALO, 64, LANES), shape(2 * HALO + 2 * ROWS, 64, LANES)],
        [], 1000, states, kappa, rate,
    )
    got_out, got_in = swaps(send_out, send_in)
    late, *work = call(
        inner_first_kernel,
        [shape(5, 64, LANES)] + fields + fine_coefs + [shape(*FINE_FLAT)] * 2,
        [], COST, states, kappa, rate, got_in,
    )
    got_late = swap(late, True)
    send_out2, send_in2, *work = call(
        outer_first_kernel,
        [shape(ROWS + HALO, 64, LANES), shape(17, 64, LANES)] + fields + fine_coefs + [shape(*FINE_FLAT)] * 2,
        [], COST, got_out, *work, aliases={1 + n: 2 + n for n in range(9)},
    )
    got_out2, got_in2 = swaps(send_out2, send_in2)
    field, other, *coefs, r_ext, k_ext = call(
        inner_second_kernel, fields + fine_coefs + [shape(*FINE_FLAT)] * 2,
        [], COST, got_in2, got_late, *work, aliases={2 + n: n for n in range(9)},
    )
    old, kc, rc = call(
        old_kernel,
        [shape(2, CROWS, 32, LANES), shape(*COARSE_FLAT), shape(*COARSE_FLAT)],
        [FINE_FIELD] + COARSE_COEFS + [COARSE_FIELD] * 2,
        COST, states, got_out, got_in, k_ext, r_ext,
    )
    field, other, send3 = call(
        outer_second_kernel,
        fields + [shape(6, 32, LANES)],
        [], COST, got_out2, field, other, *coefs, r_ext, old, aliases={1: 0, 2: 1},
    )
    got_out3, got_in3 = swaps(send3, send3)
    rc2, *coarse = call(
        chain_coefs_kernel, [shape(*COARSE_FLAT)] + coarse_coefs, [COARSE_FLAT],
        COST, kc, rc, got_late, got_in2,
    )
    tm_mid, tm_out, tm_in, first, newer = call(
        third_kernel,
        [shape(4, 32, LANES), shape(2, 32, LANES), shape(2, 32, LANES), shape(10, 32, LANES), shape(CROWS, 32, LANES)],
        [COARSE_FIELD] * 2,
        COST, send3, got_out3, got_in3, rc2, *coarse,
    )
    from_out = over_tm(tm_out, True)
    from_in = over_tm(tm_in, False)
    mid = over_tm(tm_mid, None)
    (ends,) = call(
        last_kernel,
        [shape(2, ROWS, 64, LANES)],
        [COARSE_FIELD] * 2,
        COST, field, old, first, newer, mid, from_out, from_in, rc2, *coarse,
    )
    return ends


def solution(mesh):
    in_specs = (P("tm", "space", None, None), P("space", None, None), P("space", None, None))
    out_specs = P("tm", "space", None, None)
    return jax.shard_map(shards, mesh=mesh, in_specs=in_specs, out_specs=out_specs, check_vma=False)
```

```python
import jax
import jax.numpy as jnp
from jax import lax
from jax.experimental import pallas as pl
from jax.experimental.pallas import tpu as pltpu
from jax.sharding import PartitionSpec as P

F32 = jnp.float32
LANES = 128
PAD = 8
ROWS = 8
BASE = 8
EXT = 24
CROWS = 4
CBASE = 8
CEXT = 20
HALO = 6


def lanes_of(shape):
    return lax.broadcasted_iota(jnp.int32, shape, len(shape) - 1)


def spin(value, shift):
    return pltpu.roll(value, shift % LANES, 1)


def coef_tile(i, m, k_ref, r_ref, coefs, zs):
    diag, cx, cy, cz, cw = coefs
    y = PAD + 8 * m
    k = k_ref[i, y : y + 8, :]
    k_next = k_ref[i + 1, y : y + 8, :]
    k_prev = k_ref[i - 1, y : y + 8, :]
    lane = lanes_of(k.shape)
    x_next = 0.5 * (k + k_next)
    x_prev = 0.5 * (k + k_prev)
    y_next = 0.5 * (k + k_ref[i, y + 1 : y + 9, :])
    y_prev = 0.5 * (k + k_ref[i, y - 1 : y + 7, :])
    z_next = jnp.where(lane < LANES - zs, 0.5 * (k + spin(k, -zs)), 0.0)
    z_prev = jnp.where(lane >= zs, 0.5 * (k + spin(k, zs)), 0.0)
    edge = jnp.where((lane < zs) | (lane >= LANES - zs), 0.5 * k, 0.0)
    total = x_next + x_prev + y_next + y_prev + z_next + z_prev + edge
    diag[i, 8 * m : 8 * m + 8, :] = 1.0 + r_ref[i, y : y + 8, :] - total
    cx[i, 8 * m : 8 * m + 8, :] = jnp.where(jnp.minimum(k, k_next) > 0.0, x_next, 0.0)
    cy[i, y : y + 8, :] = y_next
    cz[i, 8 * m : 8 * m + 8, :] = z_next
    cw[i, 8 * m : 8 * m + 8, :] = z_prev


def blocks(count, unroll, block):
    if count <= unroll:
        block(0, count)
        return
    trips = -(-count // unroll)
    rows = -(-count // trips)
    whole = count // rows

    def body(j, carry):
        block(j * rows, rows)
        return carry

    lax.fori_loop(0, whole, body, 0)
    if count - whole * rows:
        block(whole * rows, count - whole * rows)


def build_coefs(k_ref, r_ref, coefs, lo, count, height, zs):
    _, cx, cy, _, _ = coefs
    for m in range(height // 8):
        y = PAD + 8 * m
        k = k_ref[lo - 1, y : y + 8, :]
        k_next = k_ref[lo, y : y + 8, :]
        cx[lo - 1, 8 * m : 8 * m + 8, :] = jnp.where(
            jnp.minimum(k, k_next) > 0.0, 0.5 * (k + k_next), 0.0
        )

    def block(first, rows):
        for i in range(rows):
            cy[lo + first + i, 0:PAD, :] = jnp.zeros((PAD, LANES), F32)
            for m in range(height // 8):
                coef_tile(lo + first + i, m, k_ref, r_ref, coefs, zs)

    blocks(count, 8 if height == 64 else 14, block)


def advance(src, dst, coefs, r_ref, lo, count, height, zs, windows, unroll=8):
    diag, cx, cy, cz, cw = coefs

    def block(first, rows):
        base = lo + first
        for m in range(height // 8):
            y = PAD + 8 * m
            here = slice(y, y + 8)
            tile = slice(8 * m, 8 * m + 8)
            line = [[src[w, base + i, here, :] for i in range(-1, rows + 1)] for w in range(windows)]
            across = [cx[base + i, tile, :] for i in range(-1, rows)]
            for i in range(rows):
                row = base + i
                a = diag[row, tile, :]
                r = r_ref[row, here, :]
                y_next, y_prev = cy[row, here, :], cy[row, y - 1 : y + 7, :]
                z_next, z_prev = cz[row, tile, :], cw[row, tile, :]
                for w in range(windows):
                    u = line[w][i + 1]
                    out = u * (a - r * (u * u))
                    out = out + (across[i + 1] * line[w][i + 2] + across[i] * line[w][i])
                    out = out + (y_next * src[w, row, y + 1 : y + 9, :] + y_prev * src[w, row, y - 1 : y + 7, :])
                    out = out + (z_next * spin(u, -zs) + z_prev * spin(u, zs))
                    dst[w, row, here, :] = out

    blocks(count, unroll, block)


def clear_pads(ref, lo, hi, height):
    zero = jnp.zeros((PAD, LANES), F32)

    def body(i, carry):
        for lead in range(ref.shape[0]):
            ref[lead, i, 0:PAD, :] = zero
            ref[lead, i, PAD + height : 2 * PAD + height, :] = zero
        return carry

    lax.fori_loop(lo, hi, body, 0)


def clear_pads_flat(ref, lo, hi, height):
    zero = jnp.zeros((PAD, LANES), F32)

    def body(i, carry):
        ref[i, 0:PAD, :] = zero
        ref[i, PAD + height : 2 * PAD + height, :] = zero
        return carry

    lax.fori_loop(lo, hi, body, 0)


def pair_lanes(e):
    even = lanes_of(e.shape) % 2 == 0
    return e + jnp.where(even, spin(e, -1), spin(e, 1))


def coarse_row(load):
    return 0.125 * pair_lanes((load(0, 0) + load(0, 1)) + (load(1, 0) + load(1, 1)))


def pack2(a, b):
    return jnp.where(lanes_of(a.shape) % 2 == 0, a, b)


def unpack_a(v):
    return jnp.where(lanes_of(v.shape) % 2 == 0, v, spin(v, 1))


def unpack_b(v):
    return jnp.where(lanes_of(v.shape) % 2 == 0, spin(v, -1), v)


def odd_here():
    return lax.axis_index("space") % 2


def fetch(pairs, sems):
    copies = [pltpu.make_async_copy(a, b, sems.at[n]) for n, (a, b) in enumerate(pairs)]
    for copy in copies:
        copy.start()
    for copy in copies:
        copy.wait()


def pack_kernel(states, kappa, rate, send_out, send_in, sems):
    odd = odd_here()
    out, near = 2 * odd, 2 - 2 * odd
    copies = [
        (kappa.at[pl.ds(out, HALO)], send_out.at[pl.ds(2 * HALO, HALO)]),
        (rate.at[pl.ds(out, HALO)], send_out.at[pl.ds(3 * HALO, HALO)]),
        (kappa, send_in.at[pl.ds(2 * HALO, ROWS)]),
        (rate, send_in.at[pl.ds(2 * HALO + ROWS, ROWS)]),
    ]
    for w in range(2):
        copies.append((states.at[w, pl.ds(out, HALO)], send_out.at[pl.ds(HALO * w, HALO)]))
        copies.append((states.at[w, pl.ds(near, HALO)], send_in.at[pl.ds(HALO * w, HALO)]))
    fetch(copies, sems)


def place_halo(got, field, k_ext, r_ext, above, depth):
    for w in range(2):

        def halo(i, carry):
            field[w, 2 + 14 * above + i, PAD : PAD + 64, :] = got[HALO * w + i]
            return carry

        lax.fori_loop(0, HALO, halo, 0)
    low = 8 - depth

    def coef(i, carry):
        k_ext[low + (16 - low) * above + i, PAD : PAD + 64, :] = got[2 * HALO + i]
        r_ext[low + (16 - low) * above + i, PAD : PAD + 64, :] = got[2 * HALO + depth + i]
        return carry

    lax.fori_loop(0, depth, coef, 0)


def coarse_pair(k_ext, r_ext, fine):
    return pack2(
        coarse_row(lines_of(k_ext, (), fine)), 4.0 * coarse_row(lines_of(r_ext, (), fine))
    )


def lines_of(ref, lead, row):
    return lambda part, first: ref[lead + (row + part, pl.ds(PAD + first, 32, stride=2))]


def inner_first_kernel(
    states, kappa, rate, got_in, late, field, other, diag, cx, cy, cz, cw, r_ext, k_ext, sems
):
    odd = odd_here()
    clear_pads_flat(k_ext, 0, EXT, 64)
    clear_pads(field, 0, EXT, 64)
    clear_pads(other, 0, EXT, 64)
    rows, lines = pl.ds(BASE, ROWS), pl.ds(PAD, 64)
    fetch(
        [(states.at[w], field.at[w, rows, lines]) for w in range(2)]
        + [(kappa, k_ext.at[rows, lines]), (rate, r_ext.at[rows, lines])],
        sems,
    )
    place_halo(got_in, field, k_ext, r_ext, 1 - odd, ROWS)
    for i in range(2):
        late[i] = k_ext[BASE + 6 - 6 * odd + i, PAD : PAD + 64, :]
        late[2 + i] = r_ext[BASE + 6 - 6 * odd + i, PAD : PAD + 64, :]
        late[4, 32 * i : 32 * i + 32, :] = coarse_pair(k_ext, r_ext, 16 - 12 * odd + 2 * i)
    coefs = (diag, cx, cy, cz, cw)
    build_coefs(k_ext, r_ext, coefs, 9 - 8 * odd, 14, 64, 1)
    src, dst = field, other
    for n in range(1, 7):
        advance(src, dst, coefs, r_ext, BASE + n - 6 * odd, 14 - 2 * n, 64, 1, 2)
        src, dst = dst, src


def outer_first_kernel(got_out, *refs):
    refs = refs[9:]
    send_out, send_in, field, other, diag, cx, cy, cz, cw, r_ext, k_ext = refs
    odd = odd_here()
    place_halo(got_out, field, k_ext, r_ext, odd, HALO)
    coefs = (diag, cx, cy, cz, cw)
    build_coefs(k_ext, r_ext, coefs, 3 + 12 * odd, 6, 64, 1)
    src, dst = field, other
    for n in range(1, 7):
        advance(src, dst, coefs, r_ext, 2 + n + (14 - 2 * n) * odd, 6, 64, 1, 2)
        src, dst = dst, src

    def own(i, carry):
        for w in range(2):
            send_in[ROWS * w + i] = src[w, BASE + i, PAD : PAD + 64, :]
        send_out[i] = src[0, BASE + i, PAD : PAD + 64, :]
        return carry

    lax.fori_loop(0, ROWS, own, 0)

    def near(i, carry):
        send_out[ROWS + i] = src[1, BASE + 2 * odd + i, PAD : PAD + 64, :]
        return carry

    lax.fori_loop(0, HALO, near, 0)
    for i in range(2):
        send_in[16, 32 * i : 32 * i + 32, :] = coarse_pair(k_ext, r_ext, 4 + 12 * odd + 2 * i)


def inner_second_kernel(got_in, got_late, *refs):
    refs = refs[9:]
    field, other, diag, cx, cy, cz, cw, r_ext, k_ext = refs
    odd = odd_here()

    def halo(i, carry):
        for w in range(2):
            field[w, 16 - 16 * odd + i, PAD : PAD + 64, :] = got_in[ROWS * w + i]
        return carry

    lax.fori_loop(0, ROWS, halo, 0)
    for i in range(2):
        k_ext[22 * odd + i, PAD : PAD + 64, :] = got_late[i]
        r_ext[22 * odd + i, PAD : PAD + 64, :] = got_late[2 + i]
    coefs = (diag, cx, cy, cz, cw)
    build_coefs(k_ext, r_ext, coefs, 1 + 20 * odd, 2, 64, 1)
    src, dst = field, other
    for n in range(1, 7):
        advance(src, dst, coefs, r_ext, BASE + n - 8 * odd, 16 - 2 * n, 64, 1, 2)
        src, dst = dst, src


def outer_second_kernel(got_out, *refs):
    _, _, diag, cx, cy, cz, cw, r_ext, old, field, other, send = refs
    odd = odd_here()

    def halo(i, carry):
        field[0, 16 * odd + i, PAD : PAD + 64, :] = got_out[i]
        return carry

    def near(i, carry):
        field[1, 2 + 14 * odd + i, PAD : PAD + 64, :] = got_out[ROWS + i]
        return carry

    lax.fori_loop(0, ROWS, halo, 0)
    lax.fori_loop(0, HALO, near, 0)
    for i in range(2):
        field[1, 22 * odd + i, PAD : PAD + 64, :] = jnp.zeros((64, LANES), F32)
    coefs = (diag, cx, cy, cz, cw)
    src, dst = field, other
    for n in range(1, 7):
        advance(src, dst, coefs, r_ext, n + (16 - 2 * n) * odd, 8, 64, 1, 2)
        src, dst = dst, src
    later = (lax.axis_index("tm") > 0).astype(F32)
    for i in range(-1, 5):
        rows = []
        for w in range(2):
            value = coarse_row(lines_of(src, (w,), BASE + 2 * i))
            if 0 <= i < CROWS:
                value = value - (old[w, i] if w else later * old[w, i])
            rows.append(value)
        send[1 + i] = pack2(*rows)


def old_kernel(states, got_out, got_in, k_ext, r_ext, old, kc, rc, field, diag, cx, cy, cz, cw, here, there, sems):
    odd = odd_here()
    fetch([(states.at[w], field.at[w, pl.ds(BASE, ROWS), pl.ds(PAD, 64)]) for w in range(2)], sems)
    for got, above in ((got_out, odd), (got_in, 1 - odd)):
        for w in range(2):

            def halo(i, carry):
                field[w, 2 + 14 * above + i, PAD : PAD + 64, :] = got[HALO * w + i]
                return carry

            lax.fori_loop(0, HALO, halo, 0)
    clear_pads_flat(kc, 0, CEXT, 32)
    clear_pads(here, 0, CEXT, 32)
    clear_pads(there, 0, CEXT, 32)

    def row_coefs(first, rows):
        for i in range(rows):
            at = first + i
            kc[CBASE - 4 + at, PAD : PAD + 32, :] = coarse_row(lines_of(k_ext, (), 2 * at))
            rc[CBASE - 4 + at, PAD : PAD + 32, :] = 4.0 * coarse_row(lines_of(r_ext, (), 2 * at))

    blocks(12, 6, row_coefs)

    def row_states(first, rows):
        for i in range(rows):
            for w in range(2):
                value = coarse_row(lines_of(field, (w,), 2 + 2 * (first + i)))
                here[w, CBASE - 3 + first + i, PAD : PAD + 32, :] = value

    blocks(10, 5, row_states)
    coefs = (diag, cx, cy, cz, cw)
    build_coefs(kc, rc, coefs, CBASE - 2, CROWS + 4, 32, 2)
    src, dst = here, there
    for n in range(3):
        reach = 2 - n
        advance(src, dst, coefs, rc, CBASE - reach, CROWS + 2 * reach, 32, 2, 2)
        src, dst = dst, src
    for w in range(2):
        for i in range(CROWS):
            old[w, i] = src[w, CBASE + i, PAD : PAD + 32, :]


def chain_coefs_kernel(kc_near, rc_near, got_late, got_in2, rc, diag, cx, cy, cz, cw, kc):
    odd = odd_here()
    clear_pads_flat(kc, 0, CEXT, 32)

    def near(i, carry):
        kc[i, PAD : PAD + 32, :] = kc_near[i, PAD : PAD + 32, :]
        rc[i, PAD : PAD + 32, :] = rc_near[i, PAD : PAD + 32, :]
        return carry

    lax.fori_loop(CBASE - 4, CBASE + 8, near, 0)
    for got, slot, above in ((got_late, 4, odd), (got_in2, 16, 1 - odd)):
        for j in range(2):
            packed = got[slot, 32 * j : 32 * j + 32, :]
            row = CBASE - 6 + 14 * above + j
            kc[row, PAD : PAD + 32, :] = unpack_a(packed)
            rc[row, PAD : PAD + 32, :] = unpack_b(packed)
    build_coefs(kc, rc, (diag, cx, cy, cz, cw), CBASE - 5, CROWS + 10, 32, 2)


def third_kernel(
    sent, got_out, got_in, rc, diag, cx, cy, cz, cw,
    tm_mid, tm_out, tm_in, first, newer, here, there,
):
    odd = odd_here()
    clear_pads(here, 0, CEXT, 32)
    clear_pads(there, 0, CEXT, 32)
    coefs = (diag, cx, cy, cz, cw)
    for i in range(CROWS):
        here[0, CBASE + i, PAD : PAD + 32, :] = unpack_a(sent[1 + i])
        there[1, CBASE + i, PAD : PAD + 32, :] = unpack_b(sent[1 + i])
    for got, above in ((got_out, odd), (got_in, 1 - odd)):
        for j in range(5):
            packed = got[above + j]
            row = CBASE - 5 + 9 * above + j
            here[0, row, PAD : PAD + 32, :] = unpack_a(packed)
            there[1, row, PAD : PAD + 32, :] = unpack_b(packed)
    for i in range(-3, 7):
        first[3 + i] = here[0, CBASE + i, PAD : PAD + 32, :]
    advance(here, there, coefs, rc, CBASE - 4, CROWS + 8, 32, 2, 1, 14)
    advance(there, here, coefs, rc, CBASE - 3, CROWS + 6, 32, 2, 1, 14)
    advance(here, there, coefs, rc, CBASE - 2, CROWS + 4, 32, 2, 1, 14)
    carried = []
    for i in range(-2, 6):
        moved = there[0, CBASE + i, PAD : PAD + 32, :]
        if 0 <= i < CROWS:
            newer[i] = moved
        carried.append(moved + there[1, CBASE + i, PAD : PAD + 32, :])
    for j in range(4):
        tm_mid[j] = pack2(carried[2 * j], carried[2 * j + 1])
    for j in range(2):
        low = pack2(carried[2 * j], carried[2 * j + 1])
        high = pack2(carried[4 + 2 * j], carried[5 + 2 * j])
        tm_out[j] = jnp.where(odd > 0, low, high)
        tm_in[j] = jnp.where(odd > 0, high, low)


def last_kernel(
    fine, old, first, newer, tm_mid, from_out, from_in, rc, diag, cx, cy, cz, cw, ends, here, there
):
    clear_pads(here, 0, CEXT, 32)
    clear_pads(there, 0, CEXT, 32)
    odd = odd_here()
    for ref, start, count in ((from_out, 12 * odd - 6, 2), (tm_mid, -2, 4), (from_in, 6 - 12 * odd, 2)):
        for j in range(count):
            row = CBASE + start + 2 * j
            here[0, row, PAD : PAD + 32, :] = unpack_a(ref[j])
            here[0, row + 1, PAD : PAD + 32, :] = unpack_b(ref[j])
    coefs = (diag, cx, cy, cz, cw)
    advance(here, there, coefs, rc, CBASE - 5, CROWS + 10, 32, 2, 1, 14)
    advance(there, here, coefs, rc, CBASE - 4, CROWS + 8, 32, 2, 1, 14)
    advance(here, there, coefs, rc, CBASE - 3, CROWS + 6, 32, 2, 1, 14)
    second = []
    for i in range(-3, 7):
        moved = there[0, CBASE + i, PAD : PAD + 32, :]
        if 0 <= i < CROWS:
            second.append(moved)
        here[0, CBASE + i, PAD : PAD + 32, :] = first[3 + i] + moved
    advance(here, there, coefs, rc, CBASE - 2, CROWS + 4, 32, 2, 1, 14)
    advance(there, here, coefs, rc, CBASE - 1, CROWS + 2, 32, 2, 1, 14)
    advance(here, there, coefs, rc, CBASE, CROWS, 32, 2, 1, 14)
    later = lax.axis_index("tm") > 0
    for i in range(CROWS):
        third = there[0, CBASE + i, PAD : PAD + 32, :]
        shifts = (
            jnp.where(later, second[i] - old[0, i], 0.0),
            jnp.where(later, third, newer[i]) - old[1, i],
        )
        for w in range(2):
            for part in range(2):
                for line in range(2):
                    value = fine[w, BASE + 2 * i + part, pl.ds(PAD + line, 32, stride=2), :]
                    ends[w, 2 * i + part, pl.ds(line, 32, stride=2), :] = value + shifts[w]


def shape(*sizes):
    return jax.ShapeDtypeStruct(sizes, F32)


def call(kernel, outs, scratch, cost, *args, aliases=None, far=0, copies=0):
    spaces = [pltpu.HBM] * far + [pltpu.VMEM] * (len(args) - far)
    args = [pltpu.with_memory_space_constraint(a, pltpu.HBM) for a in args[:far]] + list(args[far:])
    return pl.pallas_call(
        kernel,
        out_shape=outs,
        in_specs=[pl.BlockSpec(memory_space=space) for space in spaces],
        out_specs=[pl.BlockSpec(memory_space=pltpu.VMEM)] * len(outs),
        scratch_shapes=[pltpu.VMEM(sizes, F32) for sizes in scratch]
        + ([pltpu.SemaphoreType.DMA((copies,))] if copies else []),
        input_output_aliases=aliases or {},
        compiler_params=pltpu.CompilerParams(vmem_limit_bytes=24 * 1024 * 1024),
        cost_estimate=pl.CostEstimate(flops=cost, bytes_accessed=1 << 20, transcendentals=0),
    )(*args)


def partners(odd_pairs):
    count = lax.axis_size("space")
    lows = range(1 if odd_pairs else 0, count - 1, 2)
    return [pair for low in lows for pair in ((low, low + 1), (low + 1, low))]


def swap(value, odd_pairs):
    count = lax.axis_size("space")
    starts = [group * count for group in range(lax.axis_size("tm"))]
    pairs = [(start + a, start + b) for start in starts for a, b in partners(odd_pairs)]
    return lax.ppermute(value, ("tm", "space"), pairs)


def over_tm(value, odd_pairs):
    count = lax.axis_size("space")
    pairs = [(s, s) for s in range(count)] if odd_pairs is None else partners(odd_pairs)
    return lax.ppermute(value, ("tm", "space"), [(a, count + b) for a, b in pairs])


FINE_COEFS = [(EXT, 64, LANES), (EXT, 64, LANES), (EXT, 64 + 2 * PAD, LANES), (EXT, 64, LANES), (EXT, 64, LANES)]
COARSE_COEFS = [(CEXT, 32, LANES), (CEXT, 32, LANES), (CEXT, 32 + 2 * PAD, LANES), (CEXT, 32, LANES), (CEXT, 32, LANES)]
FINE_FIELD = (2, EXT, 64 + 2 * PAD, LANES)
FINE_FLAT = (EXT, 64 + 2 * PAD, LANES)
COARSE_FIELD = (2, CEXT, 32 + 2 * PAD, LANES)
COARSE_FLAT = (CEXT, 32 + 2 * PAD, LANES)


def swaps(value_out, value_in):
    got_out = swap(value_out, True)
    got_in = swap(value_in, False)
    return got_out, got_in


COST = 10_000_000


def shards(states, kappa, rate):
    fields = [shape(*FINE_FIELD)] * 2
    fine_coefs = [shape(*sizes) for sizes in FINE_COEFS]
    coarse_coefs = [shape(*sizes) for sizes in COARSE_COEFS]
    send_out, send_in = call(
        pack_kernel, [shape(4 * HALO, 64, LANES), shape(2 * HALO + 2 * ROWS, 64, LANES)],
        [], 1000, states, kappa, rate, far=3, copies=8,
    )
    got_out, got_in = swaps(send_out, send_in)
    late, *work = call(
        inner_first_kernel,
        [shape(5, 64, LANES)] + fields + fine_coefs + [shape(*FINE_FLAT)] * 2,
        [], COST, states, kappa, rate, got_in, far=3, copies=4,
    )
    got_late = swap(late, True)
    send_out2, send_in2, *work = call(
        outer_first_kernel,
        [shape(ROWS + HALO, 64, LANES), shape(17, 64, LANES)] + fields + fine_coefs + [shape(*FINE_FLAT)] * 2,
        [], COST, got_out, *work, aliases={1 + n: 2 + n for n in range(9)},
    )
    got_out2, got_in2 = swaps(send_out2, send_in2)
    field, other, *coefs, r_ext, k_ext = call(
        inner_second_kernel, fields + fine_coefs + [shape(*FINE_FLAT)] * 2,
        [], COST, got_in2, got_late, *work, aliases={2 + n: n for n in range(9)},
    )
    old, kc, rc = call(
        old_kernel,
        [shape(2, CROWS, 32, LANES), shape(*COARSE_FLAT), shape(*COARSE_FLAT)],
        [FINE_FIELD] + COARSE_COEFS + [COARSE_FIELD] * 2,
        COST, states, got_out, got_in, k_ext, r_ext, far=1, copies=2,
    )
    field, other, send3 = call(
        outer_second_kernel,
        fields + [shape(6, 32, LANES)],
        [], COST, got_out2, field, other, *coefs, r_ext, old, aliases={1: 0, 2: 1},
    )
    got_out3, got_in3 = swaps(send3, send3)
    rc2, *coarse = call(
        chain_coefs_kernel, [shape(*COARSE_FLAT)] + coarse_coefs, [COARSE_FLAT],
        COST, kc, rc, got_late, got_in2,
    )
    tm_mid, tm_out, tm_in, first, newer = call(
        third_kernel,
        [shape(4, 32, LANES), shape(2, 32, LANES), shape(2, 32, LANES), shape(10, 32, LANES), shape(CROWS, 32, LANES)],
        [COARSE_FIELD] * 2,
        COST, send3, got_out3, got_in3, rc2, *coarse,
    )
    from_out = over_tm(tm_out, True)
    from_in = over_tm(tm_in, False)
    mid = over_tm(tm_mid, None)
    (ends,) = call(
        last_kernel,
        [shape(2, ROWS, 64, LANES)],
        [COARSE_FIELD] * 2,
        COST, field, old, first, newer, mid, from_out, from_in, rc2, *coarse,
    )
    return ends


def solution(mesh):
    in_specs = (P("tm", "space", None, None), P("space", None, None), P("space", None, None))
    out_specs = P("tm", "space", None, None)
    return jax.shard_map(shards, mesh=mesh, in_specs=in_specs, out_specs=out_specs, check_vma=False)
```
